256 devices in a mesh: patch: 32 (over y, x, core), rhs: 8 (over z).
Axes of the slice: x: 4, y: 4, z: 8, core: 2. Of those that a mesh axis runs over, the one named last changes fastest.
Arguments:
- rhs_vectors: float32 [256, 16, 384], P('patch', 'rhs'), may hold values from -8 to 8
- near_blocks: bfloat16 [256, 4, 384, 384], P('patch'), may hold values from -1 to 5, as said below
- neighbours: int32 [256, 4], P('patch'), may hold values from 0 to 255, as said below
- up_maps: float32 [256, 64, 384], P('patch'), may hold values from -0.3125 to 0.3125
- shift_up: float32 [256, 64, 64], P('patch'), may hold values from -0.25 to 0.25
- far_lists: int32 [32, 4], P('patch'), may hold values from 0 to 31, as said below
- translations: float32 [32, 4, 64, 64], P('patch'), may hold values from -0.375 to 0.375
- shift_down: float32 [256, 64, 64], P('patch'), may hold values from -0.75 to 0.75
- down_maps: float32 [256, 384, 64], P('patch'), may hold values from -0.375 to 0.375
Outputs:
- solution: float32 [256, 16, 384], P('patch', 'rhs')
- residual: float32 [256, 16, 384], P('patch', 'rhs')
The draws below stay inside these ranges and needn't reach their ends.
Inputs may be any that keep to these rules, and one draw needn't show every extreme that they name: `neighbours`: entry 0 of each row is the patch itself; every other entry names a patch of the same cell or of the cell just before or just after it, cyclically. `far_lists`: entry 0 of each row names the cell just before or just after the row's own cell, cyclically, and for cell 0 the cell just before it; every other entry names a cell other than the row's own. `near_blocks`: the blocks keep the operator's symmetric part positive definite.
All inputs are finite; a program needn't handle non-finite values.
Results may differ from the reference program's by a relative error of at most 0.008.
The reference program's roundings to bfloat16 on the way (of `rounded`) count: a program that leaves them out, or rounds other values in their place, can miss the bound.
Values may be sent and summed in bfloat16 or wider, within the bound.
No kernel may reach another device: no remote copies, remote signals or barrier semaphores. Data moves between devices by JAX's collectives and lax.ppermute only.
A program may use at most 64 MiB of HBM per device.

```python
import math
import jax
import jax.numpy as jnp
from jax import lax

K = 16
W = 384
E = 64
NB = 4
FL = 4
ITERS = 2
PD = 8
PATCHES = 256
CELLS = 32


def draw_near_blocks(key, part):
    spread = 0.35 / math.sqrt(W * NB)
    noise = jax.random.normal(key, (PATCHES, NB, W, W), jnp.float32) * spread
    selfpart = (jnp.arange(NB) == 0).astype(jnp.float32)[:, None, None] * jnp.eye(W, dtype=jnp.float32) * 4.0
    return (noise + selfpart[None]).astype(jnp.bfloat16)


def draw_neighbours(key, part):
    labels = jnp.arange(PATCHES, dtype=jnp.int32)
    owner = labels // PD
    offset = jax.random.randint(jax.random.fold_in(key, 11), (PATCHES, NB), 0, 3 * PD, dtype=jnp.int32) - PD
    chosen = jnp.mod(owner[:, None] * PD + offset, PATCHES).astype(jnp.int32)
    return chosen.at[:, 0].set(labels)


def draw_far_lists(key, part):
    labels = jnp.arange(CELLS, dtype=jnp.int32)
    offset = jax.random.randint(jax.random.fold_in(key, 23), (CELLS, FL), 1, CELLS, dtype=jnp.int32)
    side = jax.random.randint(jax.random.fold_in(key, 29), (CELLS,), 0, 2, dtype=jnp.int32) * 2 - 1
    side = jnp.where(labels == 0, -1, side).astype(jnp.int32)
    offset = offset.at[:, 0].set(side)
    return jnp.mod(labels[:, None] + offset, CELLS).astype(jnp.int32)


def level_of(key, dims, cuts, low, high):
    gain, own = 1.0, jax.random.fold_in(key, 6)
    for position, shards_of in cuts:
        steps = jnp.exp(jax.random.uniform(jax.random.fold_in(own, position), (shards_of,), jnp.float32, low / len(cuts), high / len(cuts)))
        gain = gain * jnp.repeat(steps, dims[position] // shards_of).reshape([-1 if axis == position else 1 for axis in range(len(dims))])
    return gain


def normal_values(rng, extent, deviation, bound, split=(), kind=jnp.bfloat16):
    loudness = level_of(rng, extent, split, -0.22, 0.18) if split else 1.0
    drawn = jax.random.normal(rng, extent, jnp.float32) * deviation * loudness
    return jnp.minimum(jnp.maximum(drawn, -bound), bound).astype(kind)


def setup_inputs(seed: int = 0) -> dict:
    seeds = jax.random.split(jax.random.key(seed), 10)
    return {
        "rhs_vectors": normal_values(seeds[0], (PATCHES, K, W), 2.0, 8.0, ((0, 32), (1, 8)), jnp.float32),
        "near_blocks": draw_near_blocks(jax.random.fold_in(seeds[9], 71), 0),
        "neighbours": draw_neighbours(jax.random.fold_in(seeds[9], 71), 0),
        "up_maps": normal_values(seeds[3], (PATCHES, E, W), W ** -0.5, 0.3125, ((0, 32),), jnp.float32),
        "shift_up": normal_values(seeds[4], (PATCHES, E, E), (E * PD) ** -0.5, 0.25, ((0, 32),), jnp.float32),
        "far_lists": draw_far_lists(jax.random.fold_in(seeds[9], 71), 0),
        "translations": normal_values(seeds[6], (CELLS, FL, E, E), (E * FL) ** -0.5, 0.375, ((0, 32),), jnp.float32),
        "shift_down": normal_values(seeds[7], (PATCHES, E, E), E ** -0.5, 0.75, ((0, 32),), jnp.float32),
        "down_maps": normal_values(seeds[8], (PATCHES, W, E), (4 * E) ** -0.5, 0.375, ((0, 32),), jnp.float32),
    }


HIGH = lax.Precision.HIGHEST

def spd_solve(matrix, right):
    factor = jnp.linalg.cholesky(matrix)
    return jax.scipy.linalg.cho_solve((factor, True), right)

def gram(left, right):
    return jnp.einsum('pkw,plw->kl', left, right, precision=HIGH)

def mix(field, coeffs):
    return jnp.einsum('pkw,kl->plw', field, coeffs, precision=HIGH)

def operator(field, near_blocks, neighbours, up_maps, shift_up, far_lists, translations, shift_down, down_maps):
    rounded = lax.optimization_barrier(field.astype(jnp.bfloat16)).astype(jnp.float32)
    picked = rounded[neighbours]
    near = jnp.einsum('pjvw,pjkw->pkv', near_blocks.astype(jnp.float32), picked, precision=HIGH)
    moments = jnp.einsum('pew,pkw->pke', up_maps, field, precision=HIGH)
    cells = moments.reshape(CELLS, PD, K, E)
    shifts = shift_up.reshape(CELLS, PD, E, E)
    cell_moment = jnp.einsum('cpfe,cpke->ckf', shifts, cells, precision=HIGH)
    sources = cell_moment[far_lists]
    local_exp = jnp.einsum('cjfe,cjke->ckf', translations, sources, precision=HIGH)
    spread = jnp.repeat(local_exp, PD, axis=0)
    patch_exp = jnp.einsum('pfe,pke->pkf', shift_down, spread, precision=HIGH)
    far = jnp.einsum('pvf,pkf->pkv', down_maps, patch_exp, precision=HIGH)
    return near + far

def reference(rhs_vectors, near_blocks, neighbours, up_maps, shift_up, far_lists, translations, shift_down, down_maps):
    residual = rhs_vectors
    solution = jnp.zeros_like(residual)
    direction = residual
    current = gram(residual, residual)
    for step in range(ITERS):
        image = operator(direction, near_blocks, neighbours, up_maps, shift_up, far_lists, translations, shift_down, down_maps)
        curve = gram(direction, image)
        curve = 0.5 * (curve + curve.T)
        alpha = spd_solve(curve, current)
        solution = solution + mix(direction, alpha)
        residual = residual - mix(image, alpha)
        if step + 1 < ITERS:
            following = gram(residual, residual)
            beta = spd_solve(current, following)
            direction = residual + mix(direction, beta)
            current = following
    return (solution, residual)
```

```python
import jax
import jax.numpy as jnp
from jax import lax
from jax.sharding import PartitionSpec as P

HIGH = lax.Precision.HIGHEST


def einsum(spec, left, right):
    return jnp.einsum(spec, left, right, precision=HIGH)


def from_everyone(array, axis):
    devices = lax.axis_size(axis)
    return lax.all_to_all(
        jnp.broadcast_to(array[None], (devices, *array.shape)), axis, 0, 0, tiled=True
    )


def collect(array, axis, dim):
    parts = jnp.moveaxis(from_everyone(array, axis), 0, dim)
    lengths = parts.shape
    return parts.reshape(*lengths[:dim], lengths[dim] * lengths[dim + 1], *lengths[dim + 2 :])


def with_halo(block, axis):
    count = lax.axis_size(axis)
    forward = [(i, (i + 1) % count) for i in range(count)]
    backward = [(target, source) for source, target in forward]
    low = lax.ppermute(block, axis, forward)
    high = lax.ppermute(block, axis, backward)
    return jnp.concatenate([low, block, high], axis=0)


def spd_solve(matrix, right):
    factor = jnp.linalg.cholesky(matrix)
    return jax.scipy.linalg.cho_solve((factor, True), right)


def gram(left, right):
    return einsum("pkw,plw->kl", left, right)


def mix(field, coeffs):
    return einsum("pkw,kl->plw", field, coeffs)


def on_device(
    rhs_vectors,
    near_blocks,
    neighbours,
    up_maps,
    shift_up,
    far_lists,
    translations,
    shift_down,
    down_maps,
):
    patches, my_cols, width = rhs_vectors.shape
    count = lax.axis_size("patch")
    offset = lax.axis_index("rhs") * my_cols
    first = lax.axis_index("patch") * patches - patches
    local_ids = jnp.mod(neighbours - first, patches * count)
    sources = far_lists[0]
    labels = jnp.arange(count, dtype=jnp.int32)
    select = (sources[:, None] == labels[None, :]).astype(jnp.float32)
    table = translations[0]

    def near_of(wide):
        picked = wide.astype(jnp.bfloat16)[local_ids]
        return jnp.einsum(
            "pjvw,pjkw->pkv", near_blocks, picked, preferred_element_type=jnp.float32
        )

    def far_of(chosen):
        local_exp = einsum("jfe,jke->kf", table, chosen)
        return einsum("pvf,kf->pkv", down, local_exp)

    up = einsum("pfe,pew->pfw", shift_up, up_maps)
    down = einsum("pve,pef->pvf", down_maps, shift_down)

    residual = collect(rhs_vectors, "rhs", 1)
    cols = residual.shape[1]
    moment = einsum("pfw,pkw->kf", up, residual)
    terms = moment.shape[1]
    pieces = from_everyone(moment, "patch")
    wide_residual = with_halo(residual, "patch")
    near = near_of(wide_residual)
    chosen = einsum("ji,ike->jke", select, pieces)
    image = near + far_of(chosen)

    image_moment = einsum("pfw,pkw->kf", up, image)
    both = jnp.concatenate([residual, image], axis=1)
    grams = gram(both, both)
    payload = jnp.concatenate(
        [grams.reshape(-1), image_moment.reshape(-1)]
    ).reshape(-1, 128)
    wide_image = with_halo(image, "patch")
    gathered = from_everyone(payload, "patch").reshape(count, -1)
    grams = gathered[:, : 4 * cols * cols].sum(axis=0).reshape(2 * cols, 2 * cols)
    image_chosen = einsum("ji,ix->jx", select, gathered[:, 4 * cols * cols :])
    image_chosen = image_chosen.reshape(-1, cols, terms)
    current = grams[:cols, :cols]
    cross = grams[:cols, cols:]
    curve = 0.5 * (cross + cross.T)
    alpha = spd_solve(curve, current)
    shared = einsum("ab,bc->ac", cross, alpha)
    following = (
        current
        - shared
        - shared.T
        + einsum("ba,bc->ac", alpha, einsum("ab,bc->ac", grams[cols:, cols:], alpha))
    )
    beta = spd_solve(current, following)
    lift = beta + jnp.eye(cols, dtype=jnp.float32)

    wide_direction = mix(wide_residual, lift) - mix(wide_image, alpha)
    direction = wide_direction[patches : 2 * patches]
    residual1 = residual - mix(image, alpha)
    chosen1 = einsum("jke,kl->jle", chosen, lift) - einsum("jke,kl->jle", image_chosen, alpha)
    image1 = near_of(wide_direction) + far_of(chosen1)
    payload = jnp.concatenate([gram(direction, image1), gram(residual1, residual1)])
    both = from_everyone(payload, "patch").sum(axis=0)
    curve = both[:cols]
    curve = 0.5 * (curve + curve.T)
    alpha1 = spd_solve(curve, both[cols:])

    mine = lax.dynamic_slice_in_dim(alpha, offset, my_cols, 1)
    mine1 = lax.dynamic_slice_in_dim(alpha1, offset, my_cols, 1)
    solution_mine = mix(residual, mine) + mix(direction, mine1)
    residual_mine = lax.dynamic_slice_in_dim(residual1, offset, my_cols, 1) - mix(image1, mine1)
    return (solution_mine, residual_mine)


def solution(mesh):
    return jax.shard_map(
        on_device,
        mesh=mesh,
        in_specs=(
            P("patch", "rhs", None),
            P("patch", None, None, None),
            P("patch", None),
            P("patch", None, None),
            P("patch", None, None),
            P("patch", None),
            P("patch", None, None, None),
            P("patch", None, None),
            P("patch", None, None),
        ),
        out_specs=(P("patch", "rhs", None), P("patch", "rhs", None)),
        check_vma=False,
    )
```

```python
import functools

import jax
import jax.numpy as jnp
from jax import lax
from jax.experimental import pallas as pl
from jax.experimental.pallas import tpu as pltpu
from jax.sharding import PartitionSpec as P

HIGH = lax.Precision.HIGHEST
F32 = jnp.float32
BF16 = jnp.bfloat16
MIB = 1024 * 1024

K = 16
W = 384
E = 64
NB = 4
FL = 4
PD = 8
ROWS = PD * K

SMEM = pl.BlockSpec(memory_space=pltpu.SMEM)
VMEM = pl.BlockSpec(memory_space=pltpu.VMEM)
ANY = pl.BlockSpec(memory_space=pl.ANY)


def shape(*dims, dtype=F32):
    return jax.ShapeDtypeStruct(dims, dtype)


def nn(left, right):
    return jnp.dot(left, right, precision=HIGH, preferred_element_type=F32)


def nt(left, right):
    return lax.dot_general(
        left, right, (((1,), (1,)), ((), ())), precision=HIGH, preferred_element_type=F32
    )


def iotas(rows, cols):
    return (
        lax.broadcasted_iota(jnp.int32, (rows, cols), 0),
        lax.broadcasted_iota(jnp.int32, (rows, cols), 1),
    )


def inverse(matrix):
    row, lane = iotas(K, 2 * K)
    eye = jnp.where(lane == row + K, 1.0, 0.0).astype(F32)
    work = jnp.concatenate([matrix, eye[:, K:]], axis=1)
    for i in range(K):
        pivot = work[i : i + 1, :] / work[i : i + 1, i : i + 1]
        work = jnp.where(row == i, pivot, work - work[:, i : i + 1] * pivot)
    return work[:, K:]


def small(left, right):
    terms = [left[:, k : k + 1] * right[k : k + 1, :] for k in range(K)]
    while len(terms) > 1:
        terms = [a + b for a, b in zip(terms[::2], terms[1::2])]
    return terms[0]


def tiled(matrix):
    wide = jnp.concatenate([matrix, jnp.zeros((K, ROWS - K), F32)], axis=1)
    for step in (K, 2 * K, 4 * K):
        wide = wide + pltpu.roll(wide, step, 1)
    return wide


def block_diagonal(matrix):
    wide = jnp.concatenate([tiled(matrix)] * PD, axis=0)
    row, lane = iotas(ROWS, ROWS)
    return jnp.where(row // K == lane // K, wide, 0.0)


def side_by_side(field):
    return jnp.concatenate([field[p * K : (p + 1) * K] for p in range(PD)], axis=1)


def fetch(near_ref, blocks_ref, sems):
    copies = [
        pltpu.make_async_copy(near_ref.at[p], blocks_ref.at[p], sems.at[p]) for p in range(PD)
    ]
    for copy in copies:
        copy.start()
    return copies


def near_product(copies, ids_ref, blocks_ref, rounded_ref):
    total = None
    for p in range(PD):
        fields = jnp.concatenate([rounded_ref[ids_ref[p, j]] for j in range(NB)], axis=1)
        pieces = [fields]
        if p:
            pieces.insert(0, jnp.zeros((p * K, NB * W), BF16))
        if p + 1 < PD:
            pieces.append(jnp.zeros(((PD - 1 - p) * K, NB * W), BF16))
        fields = jnp.concatenate(pieces, axis=0)
        copies[p].wait()
        blocks = jnp.concatenate([blocks_ref[p, j] for j in range(NB)], axis=1)
        part = lax.dot_general(
            blocks, fields, (((1,), (1,)), ((), ())), preferred_element_type=F32
        )
        total = part if total is None else total + part
    return total


def far_product(down, local_exp):
    pair = jnp.concatenate([local_exp, local_exp], axis=1)
    wide = jnp.concatenate([jnp.concatenate([pair] * (PD // 2), axis=1)] * PD, axis=0)
    row, lane = iotas(ROWS, PD * E)
    return nt(down, jnp.where(row // K == lane // E, wide, 0.0))


def chosen_expansion(far_ref, gathered_ref, table):
    chosen = jnp.concatenate([gathered_ref[far_ref[0, j]] for j in range(FL)], axis=1)
    return nt(chosen, table)


def maps_kernel(up_ref, shift_up_ref, trans_ref, shift_down_ref, down_ref, up_out, table_out, down_out):
    for p in range(PD):
        up_out[:, p * W : (p + 1) * W] = nn(shift_up_ref[p], up_ref[p])
    for q in range(PD // 2):
        pair = [nn(down_ref[2 * q + i], shift_down_ref[2 * q + i]) for i in range(2)]
        down_out[:, q * 2 * E : (q + 1) * 2 * E] = jnp.concatenate(pair, axis=1)
    for j in range(FL):
        table_out[:, j * 2 * E : (j + 1) * 2 * E] = jnp.concatenate(
            [trans_ref[j], jnp.zeros((E, E), F32)], axis=1
        )


def moment_kernel(field_ref, up_ref, out_ref):
    field = side_by_side(field_ref[...].reshape(ROWS, W))
    moment = nt(field, up_ref[...])
    message = jnp.concatenate([moment, jnp.zeros((K, E), F32)], axis=1)
    for i in range(out_ref.shape[0]):
        out_ref[i] = message


def near_kernel(ids_ref, low_ref, own_ref, high_ref, near_ref, out_ref, blocks_ref, rounded_ref, sems):
    copies = fetch(near_ref, blocks_ref, sems)
    for i, ref in enumerate((low_ref, own_ref, high_ref)):
        rounded_ref[i * PD : (i + 1) * PD] = ref[...].astype(BF16)
    out_ref[...] = near_product(copies, ids_ref, blocks_ref, rounded_ref)


def image_kernel(far_ref, gathered_ref, near_ref, field_ref, up_ref, table_ref, down_ref, image_out, local_out, out_ref):
    local_exp = chosen_expansion(far_ref, gathered_ref, table_ref[...])
    local_out[...] = jnp.concatenate([local_exp, jnp.zeros((K, E), F32)], axis=1)
    image = (near_ref[...] + far_product(down_ref[...], local_exp)).T
    image_out[...] = image.reshape(PD, K, W)
    field = side_by_side(field_ref[...].reshape(ROWS, W))
    image = side_by_side(image)
    both = jnp.concatenate([field, image], axis=0)
    grams = nt(both, both)
    moment = nt(image, up_ref[...])
    message = jnp.concatenate(
        [moment, grams[K:, :], grams[:K, :]], axis=1
    )
    for i in range(out_ref.shape[0]):
        out_ref[i] = message


def total_of(gathered_ref):
    parts = [gathered_ref[i] for i in range(gathered_ref.shape[0])]
    while len(parts) > 1:
        parts = [a + b for a, b in zip(parts[::2], parts[1::2])]
    return parts[0]


def direction_kernel(
    ids_ref, far_ref, gathered_ref, f_low, f_own, f_high, q_low, q_own, q_high,
    local_ref, table_ref, down_ref, near_ref,
    out_ref, direction_out, image_out, alpha_out,
    blocks_ref, rounded_ref, sems,
):
    copies = fetch(near_ref, blocks_ref, sems)
    total = total_of(gathered_ref)
    qr = total[:, E : E + K]
    qq = total[:, E + K : E + 2 * K]
    rr = total[:, E + 2 * K : E + 3 * K]
    rq = total[:, E + 3 * K :]
    image_exp = chosen_expansion(far_ref, gathered_ref, table_ref[...])
    curve_inv = inverse(0.5 * (qr + rq))
    rr_inv = inverse(rr)
    alpha = small(curve_inv, rr)
    alpha_t = small(rr, curve_inv)
    following = (
        rr - small(rq, alpha) - small(alpha_t, qr) + small(alpha_t, small(qq, alpha))
    )
    row, lane = iotas(K, K)
    lift_t = small(following, rr_inv) + jnp.where(row == lane, 1.0, 0.0)
    alpha_out[...] = jnp.concatenate([alpha_t, jnp.zeros((K, ROWS - K), F32)], axis=1)
    local_exp = small(lift_t, local_ref[:, :E]) - small(alpha_t, image_exp)

    coeffs = block_diagonal(-alpha_t)
    both = jnp.concatenate([block_diagonal(lift_t), coeffs], axis=1)
    for i, (f, q) in enumerate(((f_low, q_low), (f_own, q_own), (f_high, q_high))):
        pair = jnp.concatenate(
            [f[...].reshape(ROWS, W), q[...].reshape(ROWS, W)], axis=0
        )
        mixed = nn(both, pair)
        if i == 1:
            direction = mixed
            residual = f_own[...].reshape(ROWS, W) + nn(coeffs, q_own[...].reshape(ROWS, W))
        rounded_ref[i * PD : (i + 1) * PD] = mixed.astype(BF16).reshape(PD, K, W)
    direction_out[...] = direction
    image = near_product(copies, ids_ref, blocks_ref, rounded_ref)
    image = (image + far_product(down_ref[...], local_exp)).T
    image_out[...] = image
    residual = side_by_side(residual)
    grams = nt(
        jnp.concatenate([side_by_side(image), residual], axis=0),
        jnp.concatenate([side_by_side(direction), residual], axis=0),
    )
    message = jnp.concatenate(
        [grams[:K, :K], grams[K:, K:], jnp.zeros((K, ROWS - 2 * K), F32)], axis=1
    )
    for i in range(out_ref.shape[0]):
        out_ref[i] = message


def own_coeffs(place, coeffs_t):
    row, lane = iotas(K, K)
    pick = jnp.where(lane == (row % 2) * PD + place, 1.0, 0.0).astype(F32)
    row, lane = iotas(K, ROWS)
    return jnp.where(row // 2 == lane // K, tiled(small(pick, coeffs_t)), 0.0)


def first_step_kernel(place_ref, alpha_ref, field_ref, image_ref, mine_ref, x_out, r_out):
    coeffs = own_coeffs(place_ref[0], alpha_ref[:, :K])
    x_out[...] = nn(coeffs, field_ref[...].reshape(ROWS, W))
    r_out[...] = mine_ref[...].reshape(2 * PD, W) - nn(coeffs, image_ref[...].reshape(ROWS, W))


def last_step_kernel(place_ref, gathered_ref, direction_ref, image_ref, x_ref, r_ref, x_out, r_out):
    total = total_of(gathered_ref)
    qd = total[:, :K]
    alpha_t = small(total[:, K : 2 * K], inverse(0.5 * (qd + qd.T)))
    coeffs = own_coeffs(place_ref[0], alpha_t)
    x = x_ref[...] + nn(coeffs, direction_ref[...])
    r = r_ref[...] - nn(coeffs, image_ref[...])
    for p in range(PD):
        x_out[p] = x[2 * p : 2 * p + 2]
        r_out[p] = r[2 * p : 2 * p + 2]


def call(kernel, in_specs, out_shape, scratch=(), limit=24, cost=1):
    many = isinstance(out_shape, (tuple, list))
    return pl.pallas_call(
        kernel,
        in_specs=in_specs,
        out_specs=tuple(VMEM for _ in out_shape) if many else VMEM,
        out_shape=out_shape,
        scratch_shapes=scratch,
        compiler_params=pltpu.CompilerParams(vmem_limit_bytes=limit * MIB),
        cost_estimate=pl.CostEstimate(flops=cost * 1_000_000, bytes_accessed=1_000_000, transcendentals=0),
        name=kernel.__name__,
    )


NEAR_SCRATCH = (
    pltpu.VMEM((PD, NB, W, W), BF16),
    pltpu.VMEM((3 * PD, K, W), BF16),
    pltpu.SemaphoreType.DMA((PD,)),
)


def swap(array, axis):
    return lax.all_to_all(array, axis, 0, 0, tiled=True)


def halo(block, axis):
    count = lax.axis_size(axis)
    forward = [(i, (i + 1) % count) for i in range(count)]
    backward = [(target, source) for source, target in forward]
    return lax.ppermute(block, axis, forward), lax.ppermute(block, axis, backward)


def on_device(
    rhs_vectors,
    near_blocks,
    neighbours,
    up_maps,
    shift_up,
    far_lists,
    translations,
    shift_down,
    down_maps,
):
    count = lax.axis_size("patch")
    depth = lax.axis_size("rhs")
    place = lax.axis_index("rhs").astype(jnp.int32).reshape(1)
    first = lax.axis_index("patch") * PD - PD
    ids = jnp.mod(neighbours - first, PD * count)

    parts = swap(jnp.broadcast_to(rhs_vectors[None], (depth, *rhs_vectors.shape)), "rhs")
    field = parts.transpose(1, 2, 0, 3).reshape(PD, K, W)

    up, table, down = call(
        maps_kernel,
        [VMEM] * 5,
        (shape(E, PD * W), shape(E, FL * 2 * E), shape(W, PD * E)),
    )(up_maps, shift_up, translations[0], shift_down, down_maps)

    message = call(moment_kernel, [VMEM] * 2, shape(count, K, ROWS))(field, up)
    f_low, f_high = halo(field, "patch")
    gathered = swap(message, "patch")
    near = call(near_kernel, [SMEM] + [VMEM] * 3 + [ANY], shape(W, ROWS), NEAR_SCRATCH)(
        ids, f_low, field, f_high, near_blocks
    )
    image, local_exp, message = call(
        image_kernel,
        [SMEM] + [VMEM] * 6,
        (shape(PD, K, W), shape(K, 2 * E), shape(count, K, ROWS)),
    )(far_lists, gathered, near, field, up, table, down)

    q_low, q_high = halo(image, "patch")
    gathered = swap(message, "patch")
    message, direction, image1, alpha = call(
        direction_kernel,
        [SMEM] * 2 + [VMEM] * 10 + [ANY],
        (shape(count, K, ROWS), shape(ROWS, W), shape(ROWS, W), shape(K, ROWS)),
        NEAR_SCRATCH,
    )(
        ids, far_lists, gathered, f_low, field, f_high, q_low, image, q_high,
        local_exp, table, down, near_blocks,
    )

    gathered = swap(message, "patch")
    x, r = call(first_step_kernel, [SMEM] + [VMEM] * 4, (shape(2 * PD, W),) * 2)(
        place, alpha, field, image, rhs_vectors.reshape(2 * PD, W)
    )
    return call(last_step_kernel, [SMEM] + [VMEM] * 5, (shape(PD, 2, W),) * 2)(
        place, gathered, direction, image1, x, r
    )


def solution(mesh):
    return jax.shard_map(
        on_device,
        mesh=mesh,
        in_specs=(
            P("patch", "rhs", None),
            P("patch", None, None, None),
            P("patch", None),
            P("patch", None, None),
            P("patch", None, None),
            P("patch", None),
            P("patch", None, None, None),
            P("patch", None, None),
            P("patch", None, None),
        ),
        out_specs=(P("patch", "rhs", None), P("patch", "rhs", None)),
        check_vma=False,
    )
```

```python
import jax
import jax.numpy as jnp
from jax import lax
from jax.experimental import pallas as pl
from jax.experimental.pallas import tpu as pltpu
from jax.sharding import PartitionSpec as P


HIGH = lax.Precision.HIGHEST
F32 = jnp.float32
BF16 = jnp.bfloat16
MIB = 1024 * 1024

K = 16
W = 384
E = 64
NB = 4
FL = 4
PD = 8
ROWS = PD * K

SMEM = pl.BlockSpec(memory_space=pltpu.SMEM)
VMEM = pl.BlockSpec(memory_space=pltpu.VMEM)
HBM = pl.BlockSpec(memory_space=pltpu.HBM)


def shape(*dims, dtype=F32):
    return jax.ShapeDtypeStruct(dims, dtype)


def nn(left, right):
    return jnp.dot(left, right, precision=HIGH, preferred_element_type=F32)


def nt(left, right):
    return lax.dot_general(
        left, right, (((1,), (1,)), ((), ())), precision=HIGH, preferred_element_type=F32
    )


def iotas(rows, cols):
    return (
        lax.broadcasted_iota(jnp.int32, (rows, cols), 0),
        lax.broadcasted_iota(jnp.int32, (rows, cols), 1),
    )


def inverse(matrix):
    row, lane = iotas(K, 2 * K)
    eye = jnp.where(lane == row + K, 1.0, 0.0).astype(F32)
    work = jnp.concatenate([matrix, eye[:, K:]], axis=1)
    for i in range(K):
        pivot = work[i : i + 1, :] / work[i : i + 1, i : i + 1]
        work = jnp.where(row == i, pivot, work - work[:, i : i + 1] * pivot)
    return work[:, K:]


def small(left, right):
    terms = [left[:, k : k + 1] * right[k : k + 1, :] for k in range(K)]
    while len(terms) > 1:
        terms = [a + b for a, b in zip(terms[::2], terms[1::2])]
    return terms[0]


def tiled(matrix):
    wide = jnp.concatenate([matrix, jnp.zeros((K, ROWS - K), F32)], axis=1)
    for step in (K, 2 * K, 4 * K):
        wide = wide + pltpu.roll(wide, step, 1)
    return wide


def block_diagonal(matrix):
    wide = jnp.concatenate([tiled(matrix)] * PD, axis=0)
    row, lane = iotas(ROWS, ROWS)
    return jnp.where(row // K == lane // K, wide, 0.0)


def side_by_side(field):
    return jnp.concatenate([field[p * K : (p + 1) * K] for p in range(PD)], axis=1)


def fetch(near_ref, blocks_ref, sems):
    copies = [
        pltpu.make_async_copy(near_ref.at[p], blocks_ref.at[p], sems.at[p]) for p in range(PD)
    ]
    for copy in copies:
        copy.start()
    return copies


def near_product(copies, ids_ref, blocks_ref, rounded_ref):
    total = None
    for p in range(PD):
        fields = jnp.concatenate([rounded_ref[ids_ref[p, j]] for j in range(NB)], axis=1)
        pieces = [fields]
        if p:
            pieces.insert(0, jnp.zeros((p * K, NB * W), BF16))
        if p + 1 < PD:
            pieces.append(jnp.zeros(((PD - 1 - p) * K, NB * W), BF16))
        fields = jnp.concatenate(pieces, axis=0)
        copies[p].wait()
        blocks = jnp.concatenate([blocks_ref[p, j] for j in range(NB)], axis=1)
        part = lax.dot_general(
            blocks, fields, (((1,), (1,)), ((), ())), preferred_element_type=F32
        )
        total = part if total is None else total + part
    return total


def far_product(down, local_exp):
    pair = jnp.concatenate([local_exp, local_exp], axis=1)
    wide = jnp.concatenate([jnp.concatenate([pair] * (PD // 2), axis=1)] * PD, axis=0)
    row, lane = iotas(ROWS, PD * E)
    return nt(down, jnp.where(row // K == lane // E, wide, 0.0))


def chosen_expansion(far_ref, gathered_ref, table):
    chosen = []
    for j in range(FL):
        moment = gathered_ref[far_ref[0, j]]
        if moment.shape[0] < K:
            moment = jnp.concatenate([moment, pltpu.roll(moment, E, 1)], axis=0)
        chosen.append(moment)
    return nt(jnp.concatenate(chosen, axis=1), table)


def spread_kernel(mine_ref, out_ref, sem):
    copies = [
        pltpu.make_async_copy(mine_ref, out_ref.at[i], sem.at[i]) for i in range(out_ref.shape[0])
    ]
    for copy in copies:
        copy.start()
    for copy in copies:
        copy.wait()


def maps_kernel(
    up_hbm, shift_up_hbm, trans_hbm, shift_down_hbm, down_hbm,
    up_out, table_out, down_out,
    up_ref, shift_up_ref, trans_ref, shift_down_ref, down_ref, sems,
):
    pairs = (
        (up_hbm, up_ref),
        (shift_up_hbm, shift_up_ref),
        (trans_hbm, trans_ref),
        (shift_down_hbm, shift_down_ref),
        (down_hbm, down_ref),
    )
    copies = [
        pltpu.make_async_copy(source, target, sems.at[i]) for i, (source, target) in enumerate(pairs)
    ]
    for copy in copies:
        copy.start()
    for copy in copies:
        copy.wait()
    for p in range(PD):
        up_out[:, p * W : (p + 1) * W] = nn(shift_up_ref[p], up_ref[p])
    for q in range(PD // 2):
        pair = [nn(down_ref[2 * q + i].T, shift_down_ref[2 * q + i]) for i in range(2)]
        down_out[:, q * 2 * E : (q + 1) * 2 * E] = jnp.concatenate(pair, axis=1)
    for j in range(FL):
        table_out[:, j * 2 * E : (j + 1) * 2 * E] = jnp.concatenate(
            [trans_ref[j], jnp.zeros((E, E), F32)], axis=1
        )


def moment_kernel(field_ref, up_ref, out_ref):
    field = side_by_side(field_ref[...].reshape(ROWS, W))
    moment = nt(field, up_ref[...])
    message = jnp.concatenate([moment[: K // 2], moment[K // 2 :]], axis=1)
    for i in range(out_ref.shape[0]):
        out_ref[i] = message


def near_kernel(ids_ref, low_ref, own_ref, high_ref, near_ref, out_ref, blocks_ref, rounded_ref, sems):
    copies = fetch(near_ref, blocks_ref, sems)
    for i, ref in enumerate((low_ref, own_ref, high_ref)):
        rounded_ref[i * PD : (i + 1) * PD] = ref[...].astype(BF16)
    out_ref[...] = near_product(copies, ids_ref, blocks_ref, rounded_ref)


def image_kernel(far_ref, gathered_ref, near_ref, table_ref, down_ref, image_out, local_out):
    local_exp = chosen_expansion(far_ref, gathered_ref, table_ref[...])
    local_out[...] = jnp.concatenate([local_exp, jnp.zeros((K, E), F32)], axis=1)
    image = (near_ref[...] + far_product(down_ref[...], local_exp)).T
    image_out[...] = image.reshape(PD, K, W)


def grams_kernel(field_ref, image_ref, up_ref, out_ref):
    field = side_by_side(field_ref[...].reshape(ROWS, W))
    image = side_by_side(image_ref[...].reshape(ROWS, W))
    both = jnp.concatenate([field, image], axis=0)
    grams = nt(both, both)
    moment = nt(image, up_ref[...])
    message = jnp.concatenate(
        [moment, grams[K:, :], grams[:K, :]], axis=1
    )
    for i in range(out_ref.shape[0]):
        out_ref[i] = message


def total_of(gathered_ref):
    parts = [gathered_ref[i] for i in range(gathered_ref.shape[0])]
    while len(parts) > 1:
        parts = [a + b for a, b in zip(parts[::2], parts[1::2])]
    return parts[0]


def direction_kernel(
    ids_ref, far_ref, gathered_ref, f_low, f_own, f_high, q_low, q_own, q_high,
    local_ref, table_ref, down_ref, near_ref,
    out_ref, direction_out, image_out, alpha_out,
    blocks_ref, rounded_ref, sems,
):
    copies = fetch(near_ref, blocks_ref, sems)
    total = total_of(gathered_ref)
    qr = total[:, E : E + K]
    qq = total[:, E + K : E + 2 * K]
    rr = total[:, E + 2 * K : E + 3 * K]
    rq = total[:, E + 3 * K :]
    image_exp = chosen_expansion(far_ref, gathered_ref, table_ref[...])
    curve_inv = inverse(0.5 * (qr + rq))
    rr_inv = inverse(rr)
    alpha = small(curve_inv, rr)
    alpha_t = small(rr, curve_inv)
    following = (
        rr - small(rq, alpha) - small(alpha_t, qr) + small(alpha_t, small(qq, alpha))
    )
    row, lane = iotas(K, K)
    lift_t = small(following, rr_inv) + jnp.where(row == lane, 1.0, 0.0)
    alpha_out[...] = jnp.concatenate([alpha_t, jnp.zeros((K, ROWS - K), F32)], axis=1)
    local_exp = small(lift_t, local_ref[:, :E]) - small(alpha_t, image_exp)

    coeffs = block_diagonal(-alpha_t)
    both = jnp.concatenate([block_diagonal(lift_t), coeffs], axis=1)
    for i, (f, q) in enumerate(((f_low, q_low), (f_own, q_own), (f_high, q_high))):
        pair = jnp.concatenate(
            [f[...].reshape(ROWS, W), q[...].reshape(ROWS, W)], axis=0
        )
        mixed = nn(both, pair)
        if i == 1:
            direction = mixed
            residual = f_own[...].reshape(ROWS, W) + nn(coeffs, q_own[...].reshape(ROWS, W))
        rounded_ref[i * PD : (i + 1) * PD] = mixed.astype(BF16).reshape(PD, K, W)
    direction_out[...] = direction
    image = near_product(copies, ids_ref, blocks_ref, rounded_ref)
    image = (image + far_product(down_ref[...], local_exp)).T
    image_out[...] = image
    residual = side_by_side(residual)
    grams = nt(
        jnp.concatenate([side_by_side(image), residual], axis=0),
        jnp.concatenate([side_by_side(direction), residual], axis=0),
    )
    message = jnp.concatenate([grams[:K, :K], grams[K:, K:]], axis=1)
    message = jnp.concatenate(
        [message[: K // 2], message[K // 2 :], jnp.zeros((K // 2, ROWS - 4 * K), F32)], axis=1
    )
    for i in range(out_ref.shape[0]):
        out_ref[i] = message


def own_coeffs(place, coeffs_t):
    row, lane = iotas(K, K)
    pick = jnp.where(lane == (row % 2) * PD + place, 1.0, 0.0).astype(F32)
    row, lane = iotas(K, ROWS)
    return jnp.where(row // 2 == lane // K, tiled(small(pick, coeffs_t)), 0.0)


def last_step_kernel(
    place_ref, gathered_ref, alpha_ref, field_ref, image0_ref, direction_ref, image_ref,
    x_out, r_out,
):
    total = total_of(gathered_ref)
    total = jnp.concatenate([total[:, : 2 * K], total[:, 2 * K : 4 * K]], axis=0)
    qd = total[:, :K]
    row, lane = iotas(K, K)
    eye = jnp.where(row == lane, 1.0, 0.0).astype(F32)
    field = field_ref[...].reshape(ROWS, W)
    mine = own_coeffs(place_ref[0], eye)
    coeffs0 = own_coeffs(place_ref[0], alpha_ref[:, :K])
    x = nn(coeffs0, field)
    r = nn(mine, field) - nn(coeffs0, image0_ref[...].reshape(ROWS, W))
    alpha_t = small(total[:, K : 2 * K], inverse(0.5 * (qd + qd.T)))
    coeffs = own_coeffs(place_ref[0], alpha_t)
    x = x + nn(coeffs, direction_ref[...])
    r = r - nn(coeffs, image_ref[...])
    for p in range(PD):
        x_out[p] = x[2 * p : 2 * p + 2]
        r_out[p] = r[2 * p : 2 * p + 2]


def call(kernel, in_specs, out_shape, scratch=(), limit=24, cost=1):
    many = isinstance(out_shape, (tuple, list))
    return pl.pallas_call(
        kernel,
        in_specs=in_specs,
        out_specs=tuple(VMEM for _ in out_shape) if many else VMEM,
        out_shape=out_shape,
        scratch_shapes=scratch,
        compiler_params=pltpu.CompilerParams(vmem_limit_bytes=limit * MIB),
        cost_estimate=pl.CostEstimate(flops=cost * 1_000_000, bytes_accessed=1_000_000, transcendentals=0),
    )


NEAR_SCRATCH = (
    pltpu.VMEM((PD, NB, W, W), BF16),
    pltpu.VMEM((3 * PD, K, W), BF16),
    pltpu.SemaphoreType.DMA((PD,)),
)


def swap(array, axis):
    return lax.all_to_all(array, axis, 0, 0, tiled=True)


def halo(block, axis):
    count = lax.axis_size(axis)
    forward = [(i, (i + 1) % count) for i in range(count)]
    backward = [(target, source) for source, target in forward]
    return lax.ppermute(block, axis, forward), lax.ppermute(block, axis, backward)


def on_device(
    rhs_vectors,
    near_blocks,
    neighbours,
    up_maps,
    shift_up,
    far_lists,
    translations,
    shift_down,
    down_maps,
):
    count = lax.axis_size("patch")
    depth = lax.axis_size("rhs")
    place = lax.axis_index("rhs").astype(jnp.int32).reshape(1)
    first = lax.axis_index("patch") * PD - PD
    ids = jnp.mod(neighbours - first, PD * count)

    message = call(
        spread_kernel,
        [HBM],
        shape(depth, PD, 2, W),
        (pltpu.SemaphoreType.DMA((depth,)),),
        limit=63,
    )(rhs_vectors)
    parts = swap(message, "rhs")
    field = parts.transpose(1, 2, 0, 3).reshape(PD, K, W)

    up, table, down = call(
        maps_kernel,
        [HBM] * 5,
        (
            shape(E, PD * W),
            shape(E, FL * 2 * E),
            shape(W, PD * E),
        ),
        (
            pltpu.VMEM((PD, E, W), F32),
            pltpu.VMEM((PD, E, E), F32),
            pltpu.VMEM((FL, E, E), F32),
            pltpu.VMEM((PD, E, E), F32),
            pltpu.VMEM((PD, E, W), F32),
            pltpu.SemaphoreType.DMA((5,)),
        ),
        limit=53,
    )(up_maps, shift_up, translations[0], shift_down, down_maps.transpose(0, 2, 1))

    f_low, f_high = halo(field, "patch")
    message = call(moment_kernel, [VMEM] * 2, shape(count, K // 2, ROWS))(field, up)
    gathered = swap(message, "patch")
    near = call(near_kernel, [SMEM] + [VMEM] * 3 + [HBM], shape(W, ROWS), NEAR_SCRATCH, limit=48)(
        ids, f_low, field, f_high, near_blocks
    )
    image, local_exp = call(
        image_kernel, [SMEM] + [VMEM] * 4, (shape(PD, K, W), shape(K, 2 * E))
    )(far_lists, gathered, near, table, down)

    q_low, q_high = halo(image, "patch")
    message = call(grams_kernel, [VMEM] * 3, shape(count, K, ROWS))(field, image, up)
    gathered = swap(message, "patch")
    message, direction, image1, alpha = call(
        direction_kernel,
        [SMEM] * 2 + [VMEM] * 10 + [HBM],
        (shape(count, K // 2, ROWS), shape(ROWS, W), shape(ROWS, W), shape(K, ROWS)),
        NEAR_SCRATCH,
        limit=48,
    )(
        ids, far_lists, gathered, f_low, field, f_high, q_low, image, q_high,
        local_exp, table, down, near_blocks,
    )

    gathered = swap(message, "patch")
    return call(last_step_kernel, [SMEM] + [VMEM] * 6, (shape(PD, 2, W),) * 2)(
        place, gathered, alpha, field, image, direction, image1
    )


def solution(mesh):
    return jax.shard_map(
        on_device,
        mesh=mesh,
        in_specs=(
            P("patch", "rhs", None),
            P("patch", None, None, None),
            P("patch", None),
            P("patch", None, None),
            P("patch", None, None),
            P("patch", None),
            P("patch", None, None, None),
            P("patch", None, None),
            P("patch", None, None),
        ),
        out_specs=(P("patch", "rhs", None), P("patch", "rhs", None)),
        check_vma=False,
    )
```

```python
import jax
import jax.numpy as jnp
from jax import lax
from jax.experimental import pallas as pl
from jax.experimental.pallas import tpu as pltpu
from jax.sharding import PartitionSpec as P


HIGH = lax.Precision.HIGHEST
F32 = jnp.float32
BF16 = jnp.bfloat16
MIB = 1024 * 1024

K = 16
W = 384
E = 64
NB = 4
FL = 4
PD = 8
ROWS = PD * K

SMEM = pl.BlockSpec(memory_space=pltpu.SMEM)
VMEM = pl.BlockSpec(memory_space=pltpu.VMEM)
HBM = pl.BlockSpec(memory_space=pltpu.HBM)


def shape(*dims, dtype=F32):
    return jax.ShapeDtypeStruct(dims, dtype)


def nn(left, right):
    return jnp.dot(left, right, precision=HIGH, preferred_element_type=F32)


def nt(left, right):
    return lax.dot_general(
        left, right, (((1,), (1,)), ((), ())), precision=HIGH, preferred_element_type=F32
    )


def iotas(rows, cols):
    return (
        lax.broadcasted_iota(jnp.int32, (rows, cols), 0),
        lax.broadcasted_iota(jnp.int32, (rows, cols), 1),
    )


def inverse(matrix):
    row, lane = iotas(K, 2 * K)
    eye = jnp.where(lane == row + K, 1.0, 0.0).astype(F32)
    work = jnp.concatenate([matrix, eye[:, K:]], axis=1)
    for i in range(K):
        pivot = work[i : i + 1, :] / work[i : i + 1, i : i + 1]
        work = jnp.where(row == i, pivot, work - work[:, i : i + 1] * pivot)
    return work[:, K:]


def small(left, right):
    terms = [left[:, k : k + 1] * right[k : k + 1, :] for k in range(K)]
    while len(terms) > 1:
        terms = [a + b for a, b in zip(terms[::2], terms[1::2])]
    return terms[0]


def tiled(matrix):
    wide = jnp.concatenate([matrix, jnp.zeros((K, ROWS - K), F32)], axis=1)
    for step in (K, 2 * K, 4 * K):
        wide = wide + pltpu.roll(wide, step, 1)
    return wide


def block_diagonal(matrix):
    wide = jnp.concatenate([tiled(matrix)] * PD, axis=0)
    row, lane = iotas(ROWS, ROWS)
    return jnp.where(row // K == lane // K, wide, 0.0)


def side_by_side(field):
    return jnp.concatenate([field[p * K : (p + 1) * K] for p in range(PD)], axis=1)


def fetch(near_ref, blocks_ref, sems):
    def start(p, carry):
        pltpu.make_async_copy(near_ref.at[p], blocks_ref.at[p], sems.at[p]).start()
        return carry

    lax.fori_loop(0, PD, start, 0)


def fetched(near_ref, blocks_ref, sems):
    def wait(p, carry):
        pltpu.make_async_copy(near_ref.at[p], blocks_ref.at[p], sems.at[p]).wait()
        return carry

    lax.fori_loop(0, PD, wait, 0)


def near_product(ids_ref, blocks_ref, rounded_ref):
    total = None
    for p in range(PD):
        fields = jnp.concatenate([rounded_ref[ids_ref[p, j]] for j in range(NB)], axis=1)
        pieces = [fields]
        if p:
            pieces.insert(0, jnp.zeros((p * K, NB * W), BF16))
        if p + 1 < PD:
            pieces.append(jnp.zeros(((PD - 1 - p) * K, NB * W), BF16))
        fields = jnp.concatenate(pieces, axis=0)
        blocks = jnp.concatenate([blocks_ref[p, j] for j in range(NB)], axis=1)
        part = lax.dot_general(
            blocks, fields, (((1,), (1,)), ((), ())), preferred_element_type=F32
        )
        total = part if total is None else total + part
    return total


def shifted(local_exp, shift_ref):
    return nt(local_exp, shift_ref[...].reshape(PD * E, E))


def far_product(patch_exp, down_ref):
    row, lane = iotas(ROWS, PD * E)
    wide = jnp.concatenate([patch_exp] * PD, axis=0)
    wide = jnp.where(row // K == lane // E, wide, 0.0)
    return nn(wide, down_ref[...].reshape(PD * E, W))


def chosen_expansion(far_ref, gathered_ref, table_ref):
    total = None
    for j in range(FL):
        moment = gathered_ref[far_ref[0, j]]
        if moment.shape[0] < K:
            moment = jnp.concatenate([moment[:, :E], moment[:, E:]], axis=0)
        part = nt(moment[:, :E], table_ref[j])
        total = part if total is None else total + part
    return total


def spread_kernel(mine_ref, out_ref, sem):
    copies = [
        pltpu.make_async_copy(mine_ref, out_ref.at[i], sem.at[i]) for i in range(out_ref.shape[0])
    ]
    for copy in copies:
        copy.start()
    for copy in copies:
        copy.wait()


def maps_kernel(up_ref, shift_ref, out_ref):
    for p in range(PD):
        out_ref[:, p * W : (p + 1) * W] = nn(shift_ref[p], up_ref[p])


def moment_kernel(field_ref, up_ref, out_ref):
    moment = nt(side_by_side(field_ref[...].reshape(ROWS, W)), up_ref[...])
    message = jnp.concatenate([moment[: K // 2], moment[K // 2 :]], axis=1)
    for i in range(out_ref.shape[0]):
        out_ref[i] = message


def near_kernel(ids_ref, low_ref, own_ref, high_ref, near_ref, out_ref, blocks_ref, rounded_ref, sems):
    fetch(near_ref, blocks_ref, sems)
    for i, ref in enumerate((low_ref, own_ref, high_ref)):
        rounded_ref[i * PD : (i + 1) * PD] = ref[...].astype(BF16)
    fetched(near_ref, blocks_ref, sems)
    out_ref[...] = near_product(ids_ref, blocks_ref, rounded_ref).T


def image_kernel(far_ref, gathered_ref, near_ref, table_ref, shift_ref, down_ref, image_out, local_out):
    local_exp = chosen_expansion(far_ref, gathered_ref, table_ref)
    local_out[...] = jnp.concatenate([local_exp, jnp.zeros((K, E), F32)], axis=1)
    image = near_ref[...] + far_product(shifted(local_exp, shift_ref), down_ref)
    image_out[...] = image.reshape(PD, K, W)


def grams_kernel(field_ref, image_ref, up_ref, out_ref):
    image = side_by_side(image_ref[...].reshape(ROWS, W))
    moment = nt(image, up_ref[...])
    both = jnp.concatenate([side_by_side(field_ref[...].reshape(ROWS, W)), image], axis=0)
    grams = nt(both, both)
    message = jnp.concatenate(
        [moment, grams[K:, :], grams[:K, :]], axis=1
    )
    for i in range(out_ref.shape[0]):
        out_ref[i] = message


def total_of(gathered_ref):
    parts = [gathered_ref[i] for i in range(gathered_ref.shape[0])]
    while len(parts) > 1:
        parts = [a + b for a, b in zip(parts[::2], parts[1::2])]
    return parts[0]


def direction_kernel(
    ids_ref, far_ref, gathered_ref, f_low, f_own, f_high, q_low, q_own, q_high,
    local_ref, table_ref, shift_ref, down_ref, near_ref,
    out_ref, direction_out, image_out, alpha_out,
    blocks_ref, rounded_ref, sems,
):
    fetch(near_ref, blocks_ref, sems)
    total = total_of(gathered_ref)
    qr = total[:, E : E + K]
    qq = total[:, E + K : E + 2 * K]
    rr = total[:, E + 2 * K : E + 3 * K]
    rq = total[:, E + 3 * K :]
    image_exp = chosen_expansion(far_ref, gathered_ref, table_ref)
    curve_inv = inverse(0.5 * (qr + rq))
    rr_inv = inverse(rr)
    alpha = small(curve_inv, rr)
    alpha_t = small(rr, curve_inv)
    following = (
        rr - small(rq, alpha) - small(alpha_t, qr) + small(alpha_t, small(qq, alpha))
    )
    row, lane = iotas(K, K)
    lift_t = small(following, rr_inv) + jnp.where(row == lane, 1.0, 0.0)
    alpha_out[...] = jnp.concatenate([alpha_t, jnp.zeros((K, ROWS - K), F32)], axis=1)
    local_exp = small(lift_t, local_ref[:, :E]) - small(alpha_t, image_exp)
    far = far_product(shifted(local_exp, shift_ref), down_ref)

    coeffs = block_diagonal(-alpha_t)
    both = jnp.concatenate([block_diagonal(lift_t), coeffs], axis=1)
    for i, (f, q) in enumerate(((f_low, q_low), (f_own, q_own), (f_high, q_high))):
        pair = jnp.concatenate(
            [f[...].reshape(ROWS, W), q[...].reshape(ROWS, W)], axis=0
        )
        mixed = nn(both, pair)
        if i == 1:
            direction = mixed
            residual = f_own[...].reshape(ROWS, W) + nn(coeffs, q_own[...].reshape(ROWS, W))
        rounded_ref[i * PD : (i + 1) * PD] = mixed.astype(BF16).reshape(PD, K, W)
    direction_out[...] = direction
    fetched(near_ref, blocks_ref, sems)
    image = near_product(ids_ref, blocks_ref, rounded_ref)
    image = image.T + far
    image_out[...] = image
    residual = side_by_side(residual)
    grams = nt(
        jnp.concatenate([side_by_side(image), residual], axis=0),
        jnp.concatenate([side_by_side(direction), residual], axis=0),
    )
    message = jnp.concatenate([grams[:K, :K], grams[K:, K:]], axis=1)
    message = jnp.concatenate(
        [message[: K // 2], message[K // 2 :], jnp.zeros((K // 2, ROWS - 4 * K), F32)], axis=1
    )
    for i in range(out_ref.shape[0]):
        out_ref[i] = message


def own_coeffs(place, coeffs_t):
    row, lane = iotas(K, K)
    pick = jnp.where(lane == (row % 2) * PD + place, 1.0, 0.0).astype(F32)
    row, lane = iotas(K, ROWS)
    return jnp.where(row // 2 == lane // K, tiled(small(pick, coeffs_t)), 0.0)


def last_step_kernel(
    place_ref, gathered_ref, alpha_ref, field_ref, image0_ref, direction_ref, image_ref,
    x_out, r_out,
):
    total = total_of(gathered_ref)
    total = jnp.concatenate([total[:, : 2 * K], total[:, 2 * K : 4 * K]], axis=0)
    qd = total[:, :K]
    row, lane = iotas(K, K)
    eye = jnp.where(row == lane, 1.0, 0.0).astype(F32)
    field = field_ref[...].reshape(ROWS, W)
    mine = own_coeffs(place_ref[0], eye)
    coeffs0 = own_coeffs(place_ref[0], alpha_ref[:, :K])
    x = nn(coeffs0, field)
    r = nn(mine, field) - nn(coeffs0, image0_ref[...].reshape(ROWS, W))
    alpha_t = small(total[:, K : 2 * K], inverse(0.5 * (qd + qd.T)))
    coeffs = own_coeffs(place_ref[0], alpha_t)
    x = x + nn(coeffs, direction_ref[...])
    r = r - nn(coeffs, image_ref[...])
    for p in range(PD):
        x_out[p] = x[2 * p : 2 * p + 2]
        r_out[p] = r[2 * p : 2 * p + 2]


def call(kernel, in_specs, out_shape, scratch=(), limit=24, cost=1):
    many = isinstance(out_shape, (tuple, list))
    return pl.pallas_call(
        kernel,
        in_specs=in_specs,
        out_specs=tuple(VMEM for _ in out_shape) if many else VMEM,
        out_shape=out_shape,
        scratch_shapes=scratch,
        compiler_params=pltpu.CompilerParams(vmem_limit_bytes=limit * MIB),
        cost_estimate=pl.CostEstimate(flops=cost * 1_000_000, bytes_accessed=1_000_000, transcendentals=0),
    )


NEAR_SCRATCH = (
    pltpu.VMEM((PD, NB, W, W), BF16),
    pltpu.VMEM((3 * PD, K, W), BF16),
    pltpu.SemaphoreType.DMA((PD,)),
)


def swap(array, axis):
    return lax.all_to_all(array, axis, 0, 0, tiled=True)


def halo(block, axis):
    count = lax.axis_size(axis)
    forward = [(i, (i + 1) % count) for i in range(count)]
    backward = [(target, source) for source, target in forward]
    return lax.ppermute(block, axis, forward), lax.ppermute(block, axis, backward)


def on_device(
    rhs_vectors,
    near_blocks,
    neighbours,
    up_maps,
    shift_up,
    far_lists,
    translations,
    shift_down,
    down_maps,
):
    count = lax.axis_size("patch")
    depth = lax.axis_size("rhs")
    place = lax.axis_index("rhs").astype(jnp.int32).reshape(1)
    first = lax.axis_index("patch") * PD - PD
    ids = jnp.mod(neighbours - first, PD * count)

    message = call(
        spread_kernel,
        [HBM],
        shape(depth, PD, 2, W),
        (pltpu.SemaphoreType.DMA((depth,)),),
        limit=63,
    )(rhs_vectors)
    parts = swap(message, "rhs")
    field = parts.transpose(1, 2, 0, 3).reshape(PD, K, W)

    up = call(maps_kernel, [VMEM] * 2, shape(E, PD * W))(up_maps, shift_up)
    table = translations[0]
    down = down_maps.transpose(0, 2, 1)

    f_low, f_high = halo(field, "patch")
    message = call(moment_kernel, [VMEM] * 2, shape(count, K // 2, ROWS))(field, up)
    gathered = swap(message, "patch")
    near = call(near_kernel, [SMEM] + [VMEM] * 3 + [HBM], shape(ROWS, W), NEAR_SCRATCH, limit=48)(
        ids, f_low, field, f_high, near_blocks
    )
    image, local_exp = call(
        image_kernel, [SMEM] + [VMEM] * 5, (shape(PD, K, W), shape(K, 2 * E))
    )(far_lists, gathered, near, table, shift_down, down)

    q_low, q_high = halo(image, "patch")
    message = call(grams_kernel, [VMEM] * 3, shape(count, K, ROWS))(field, image, up)
    gathered = swap(message, "patch")
    message, direction, image1, alpha = call(
        direction_kernel,
        [SMEM] * 2 + [VMEM] * 11 + [HBM],
        (shape(count, K // 2, ROWS), shape(ROWS, W), shape(ROWS, W), shape(K, ROWS)),
        NEAR_SCRATCH,
        limit=48,
    )(
        ids, far_lists, gathered, f_low, field, f_high, q_low, image, q_high,
        local_exp, table, shift_down, down, near_blocks,
    )

    gathered = swap(message, "patch")
    return call(last_step_kernel, [SMEM] + [VMEM] * 6, (shape(PD, 2, W),) * 2)(
        place, gathered, alpha, field, image, direction, image1
    )


def solution(mesh):
    return jax.shard_map(
        on_device,
        mesh=mesh,
        in_specs=(
            P("patch", "rhs", None),
            P("patch", None, None, None),
            P("patch", None),
            P("patch", None, None),
            P("patch", None, None),
            P("patch", None),
            P("patch", None, None, None),
            P("patch", None, None),
            P("patch", None, None),
        ),
        out_specs=(P("patch", "rhs", None), P("patch", "rhs", None)),
        check_vma=False,
    )
```

```python
import jax
import jax.numpy as jnp
from jax import lax
from jax.experimental import pallas as pl
from jax.experimental.pallas import tpu as pltpu
from jax.sharding import PartitionSpec as P


HIGH = lax.Precision.HIGH
F32 = jnp.float32
BF16 = jnp.bfloat16
MIB = 1024 * 1024

K = 16
W = 384
E = 64
NB = 4
FL = 4
PD = 8
ROWS = PD * K

SMEM = pl.BlockSpec(memory_space=pltpu.SMEM)
VMEM = pl.BlockSpec(memory_space=pltpu.VMEM)
HBM = pl.BlockSpec(memory_space=pltpu.HBM)


def shape(*dims, dtype=F32):
    return jax.ShapeDtypeStruct(dims, dtype)


def nn(left, right):
    return jnp.dot(left, right, precision=HIGH, preferred_element_type=F32)


def exact(left, right):
    return jnp.dot(left, right, precision=lax.Precision.HIGHEST, preferred_element_type=F32)


def nt(left, right):
    return lax.dot_general(
        left, right, (((1,), (1,)), ((), ())), precision=HIGH, preferred_element_type=F32
    )


def iotas(rows, cols):
    return (
        lax.broadcasted_iota(jnp.int32, (rows, cols), 0),
        lax.broadcasted_iota(jnp.int32, (rows, cols), 1),
    )


def inverse(matrix):
    row, lane = iotas(K, 2 * K)
    eye = jnp.where(lane == row + K, 1.0, 0.0).astype(F32)
    work = jnp.concatenate([matrix, eye[:, K:]], axis=1)
    for i in range(0, K, 2):
        left = jnp.broadcast_to(work[:, i : i + 1], (K, 2 * K))
        right = jnp.broadcast_to(work[:, i + 1 : i + 2], (K, 2 * K))
        a, c = left[i : i + 1], left[i + 1 : i + 2]
        b, d = right[i : i + 1], right[i + 1 : i + 2]
        upper, lower = work[i : i + 1], work[i + 1 : i + 2]
        scale = 1.0 / (a * d - b * c)
        upper, lower = (d * upper - b * lower) * scale, (a * lower - c * upper) * scale
        rest = work - left * upper - right * lower
        work = jnp.where(row == i, upper, jnp.where(row == i + 1, lower, rest))
    return work[:, K:]


def small(left, right):
    terms = [left[:, k : k + 1] * right[k : k + 1, :] for k in range(K)]
    while len(terms) > 1:
        terms = [a + b for a, b in zip(terms[::2], terms[1::2])]
    return terms[0]


def tiled(matrix):
    wide = jnp.concatenate([matrix, jnp.zeros((K, ROWS - K), F32)], axis=1)
    for step in (K, 2 * K, 4 * K):
        wide = wide + pltpu.roll(wide, step, 1)
    return wide


def block_diagonal(matrix):
    wide = jnp.concatenate([tiled(matrix)] * PD, axis=0)
    row, lane = iotas(ROWS, ROWS)
    return jnp.where(row // K == lane // K, wide, 0.0)


def side_by_side(field):
    return jnp.concatenate([field[p * K : (p + 1) * K] for p in range(PD)], axis=1)


def fetch(near_ref, blocks_ref, sems):
    def start(p, carry):
        pltpu.make_async_copy(near_ref.at[p], blocks_ref.at[p], sems.at[p]).start()
        return carry

    lax.fori_loop(0, PD, start, 0)


def fetched(near_ref, blocks_ref, sems):
    def wait(p, carry):
        pltpu.make_async_copy(near_ref.at[p], blocks_ref.at[p], sems.at[p]).wait()
        return carry

    lax.fori_loop(0, PD, wait, 0)


def near_product(ids_ref, blocks_ref, rounded_ref):
    total = None
    for p in range(PD):
        fields = jnp.concatenate([rounded_ref[ids_ref[p, j]] for j in range(NB)], axis=1)
        pieces = [fields]
        if p:
            pieces.insert(0, jnp.zeros((p * K, NB * W), BF16))
        if p + 1 < PD:
            pieces.append(jnp.zeros(((PD - 1 - p) * K, NB * W), BF16))
        fields = jnp.concatenate(pieces, axis=0)
        blocks = jnp.concatenate([blocks_ref[p, j] for j in range(NB)], axis=1)
        part = lax.dot_general(
            blocks, fields, (((1,), (1,)), ((), ())), preferred_element_type=F32
        )
        total = part if total is None else total + part
    return total


def shifted(local_exp, shift_ref):
    return nt(local_exp, shift_ref[...].reshape(PD * E, E))


def far_product(patch_exp, down_ref):
    row, lane = iotas(ROWS, PD * E)
    wide = jnp.concatenate([patch_exp] * PD, axis=0)
    wide = jnp.where(row // K == lane // E, wide, 0.0)
    return nn(wide, down_ref[...].reshape(PD * E, W))


def expansion(chosen, table_ref):
    total = None
    for j in range(FL):
        moment = chosen[j]
        if moment.shape[0] < K:
            moment = jnp.concatenate([moment[:, :E], moment[:, E:]], axis=0)
        part = nt(moment[:, :E], table_ref[j])
        total = part if total is None else total + part
    return total


def summed(parts):
    while len(parts) > 1:
        parts = [a + b for a, b in zip(parts[::2], parts[1::2])]
    return parts[0]


def maps_kernel(up_ref, shift_ref, out_ref):
    for p in range(PD):
        out_ref[:, p * W : (p + 1) * W] = nn(shift_ref[p], up_ref[p])


def moment_kernel(field_ref, up_ref, out_ref):
    moment = nt(side_by_side(field_ref[...].reshape(ROWS, W)), up_ref[...])
    message = jnp.concatenate([moment[: K // 2], moment[K // 2 :]], axis=1)
    for i in range(out_ref.shape[0]):
        out_ref[i] = message


def near_kernel(
    ids_ref, low_ref, own_ref, high_ref, near_ref, out_ref, blocks_ref, rounded_ref, ids_smem, sems
):
    ids = pltpu.make_async_copy(ids_ref, ids_smem, sems.at[PD])
    ids.start()
    fetch(near_ref, blocks_ref, sems)
    for i, ref in enumerate((low_ref, own_ref, high_ref)):
        rounded_ref[i * PD : (i + 1) * PD] = ref[...].astype(BF16)
    ids.wait()
    fetched(near_ref, blocks_ref, sems)
    out_ref[...] = near_product(ids_smem, blocks_ref, rounded_ref).T


def image_kernel(
    pick_ref, gathered_ref, near_ref, field_ref, up_ref, table_ref, shift_ref, down_ref,
    image_out, local_out, out_ref,
):
    count = gathered_ref.shape[0]
    chosen = [
        summed([gathered_ref[c] * pick_ref[j * count + c : j * count + c + 1] for c in range(count)])
        for j in range(FL)
    ]
    local_exp = expansion(chosen, table_ref)
    local_out[...] = jnp.concatenate([local_exp, jnp.zeros((K, E), F32)], axis=1)
    image = near_ref[...] + far_product(shifted(local_exp, shift_ref), down_ref)
    image_out[...] = image.reshape(PD, K, W)
    image = side_by_side(image)
    moment = nt(image, up_ref[...])
    both = jnp.concatenate([side_by_side(field_ref[...].reshape(ROWS, W)), image], axis=0)
    grams = nt(both, both)
    message = jnp.concatenate(
        [moment, grams[K:, :], grams[:K, :]], axis=1
    )
    for i in range(out_ref.shape[0]):
        out_ref[i] = message


def total_of(gathered_ref):
    return summed([gathered_ref[i] for i in range(gathered_ref.shape[0])])


def direction_kernel(
    ids_ref, far_ref, gathered_ref, f_low, f_own, f_high, q_low, q_own, q_high,
    local_ref, table_ref, shift_ref, down_ref, near_ref,
    out_ref, direction_out, image_out, alpha_out,
    blocks_ref, rounded_ref, ids_smem, far_smem, sems,
):
    ids = pltpu.make_async_copy(ids_ref, ids_smem, sems.at[PD])
    far_ids = pltpu.make_async_copy(far_ref, far_smem, sems.at[PD + 1])
    ids.start()
    far_ids.start()
    fetch(near_ref, blocks_ref, sems)
    total = total_of(gathered_ref)
    qr = total[:, E : E + K]
    qq = total[:, E + K : E + 2 * K]
    rr = total[:, E + 2 * K : E + 3 * K]
    rq = total[:, E + 3 * K :]
    curve_inv = inverse(0.5 * (qr + rq))
    rr_inv = inverse(rr)
    alpha = small(curve_inv, rr)
    alpha_t = small(rr, curve_inv)
    following = (
        rr - small(rq, alpha) - small(alpha_t, qr) + small(alpha_t, small(qq, alpha))
    )
    row, lane = iotas(K, K)
    lift_t = small(following, rr_inv) + jnp.where(row == lane, 1.0, 0.0)
    alpha_out[...] = jnp.concatenate([alpha_t, jnp.zeros((K, ROWS - K), F32)], axis=1)
    far_ids.wait()
    image_exp = expansion([gathered_ref[far_smem[0, j]] for j in range(FL)], table_ref)
    local_exp = small(lift_t, local_ref[:, :E]) - small(alpha_t, image_exp)
    far = far_product(shifted(local_exp, shift_ref), down_ref)

    coeffs = block_diagonal(-alpha_t)
    both = jnp.concatenate([block_diagonal(lift_t), coeffs], axis=1)
    for i, (f, q) in enumerate(((f_low, q_low), (f_own, q_own), (f_high, q_high))):
        pair = jnp.concatenate(
            [f[...].reshape(ROWS, W), q[...].reshape(ROWS, W)], axis=0
        )
        mixed = nn(both, pair)
        if i == 1:
            direction = mixed
            residual = f_own[...].reshape(ROWS, W) + nn(coeffs, q_own[...].reshape(ROWS, W))
        rounded_ref[i * PD : (i + 1) * PD] = mixed.astype(BF16).reshape(PD, K, W)
    direction_out[...] = direction
    ids.wait()
    fetched(near_ref, blocks_ref, sems)
    image = near_product(ids_smem, blocks_ref, rounded_ref)
    image = image.T + far
    image_out[...] = image
    residual = side_by_side(residual)
    grams = nt(
        jnp.concatenate([side_by_side(image), residual], axis=0),
        jnp.concatenate([side_by_side(direction), residual], axis=0),
    )
    message = jnp.concatenate([grams[:K, :K], grams[K:, K:]], axis=1)
    message = jnp.concatenate(
        [message[: K // 2], message[K // 2 :], jnp.zeros((K // 2, ROWS - 4 * K), F32)], axis=1
    )
    for i in range(out_ref.shape[0]):
        out_ref[i] = message


def own_coeffs(pick, coeffs_t):
    row, lane = iotas(K, ROWS)
    return jnp.where(row // 2 == lane // K, tiled(small(pick, coeffs_t)), 0.0)


def last_step_kernel(
    pick_ref, gathered_ref, alpha_ref, field_ref, image0_ref, direction_ref, image_ref,
    x_out, r_out,
):
    total = total_of(gathered_ref)
    total = jnp.concatenate([total[:, : 2 * K], total[:, 2 * K : 4 * K]], axis=0)
    pick = pick_ref[...]
    qd = total[:, :K]
    field = field_ref[...].reshape(ROWS, W)
    row, lane = iotas(K, ROWS)
    mine = jnp.where(row // 2 == lane // K, tiled(pick), 0.0)
    coeffs0 = own_coeffs(pick, alpha_ref[:, :K])
    x = nn(coeffs0, field)
    r = exact(mine, field) - exact(coeffs0, image0_ref[...].reshape(ROWS, W))
    alpha_t = small(total[:, K : 2 * K], inverse(0.5 * (qd + qd.T)))
    coeffs = own_coeffs(pick, alpha_t)
    x = x + nn(coeffs, direction_ref[...])
    r = r - nn(coeffs, image_ref[...])
    for p in range(PD):
        x_out[p] = x[2 * p : 2 * p + 2]
        r_out[p] = r[2 * p : 2 * p + 2]


def call(kernel, in_specs, out_shape, scratch=(), limit=24, cost=1):
    many = isinstance(out_shape, (tuple, list))
    return pl.pallas_call(
        kernel,
        in_specs=in_specs,
        out_specs=tuple(VMEM for _ in out_shape) if many else VMEM,
        out_shape=out_shape,
        scratch_shapes=scratch,
        compiler_params=pltpu.CompilerParams(vmem_limit_bytes=limit * MIB),
        cost_estimate=pl.CostEstimate(flops=cost * 1_000_000, bytes_accessed=1_000_000, transcendentals=0),
    )


NEAR_SCRATCH = (
    pltpu.VMEM((PD, NB, W, W), BF16),
    pltpu.VMEM((3 * PD, K, W), BF16),
    pltpu.SMEM((PD, NB), jnp.int32),
)


def swap(array, axis):
    return lax.all_to_all(array, axis, 0, 0, tiled=True)


def halo(block, axis):
    count = lax.axis_size(axis)
    forward = [(i, (i + 1) % count) for i in range(count)]
    backward = [(target, source) for source, target in forward]
    return lax.ppermute(block, axis, forward), lax.ppermute(block, axis, backward)


def on_device(
    rhs_vectors,
    near_blocks,
    neighbours,
    up_maps,
    shift_up,
    far_lists,
    translations,
    shift_down,
    down_maps,
):
    count = lax.axis_size("patch")
    depth = lax.axis_size("rhs")
    place = lax.axis_index("rhs").astype(jnp.int32)
    first = lax.axis_index("patch") * PD - PD
    ids = jnp.mod(neighbours - first, PD * count)

    message = jnp.broadcast_to(rhs_vectors[None], (depth, *rhs_vectors.shape))
    parts = swap(message, "rhs")
    field = parts.transpose(1, 2, 0, 3).reshape(PD, K, W)

    row, lane = jnp.arange(K)[:, None], jnp.arange(K)[None, :]
    pick_column = (lane == (row % 2) * PD + place).astype(F32)
    pick_cell = (far_lists[0][:, None] == jnp.arange(count)[None, :]).astype(F32)
    pick_cell = jnp.broadcast_to(pick_cell.reshape(FL * count, 1), (FL * count, 2 * E))

    up = call(maps_kernel, [VMEM] * 2, shape(E, PD * W))(up_maps, shift_up)
    table = translations[0]
    down = down_maps.transpose(0, 2, 1)

    f_low, f_high = halo(field, "patch")
    message = call(moment_kernel, [VMEM] * 2, shape(count, K // 2, ROWS))(field, up)
    gathered = swap(message, "patch")
    near = call(
        near_kernel,
        [VMEM] * 4 + [HBM],
        shape(ROWS, W),
        (*NEAR_SCRATCH, pltpu.SemaphoreType.DMA((PD + 1,))),
        limit=48,
    )(
        ids, f_low, field, f_high, near_blocks
    )
    image, local_exp, message = call(
        image_kernel,
        [VMEM] * 8,
        (shape(PD, K, W), shape(K, 2 * E), shape(count, K, ROWS)),
    )(pick_cell, gathered, near, field, up, table, shift_down, down)

    q_low, q_high = halo(image, "patch")
    gathered = swap(message, "patch")
    message, direction, image1, alpha = call(
        direction_kernel,
        [VMEM] * 13 + [HBM],
        (shape(count, K // 2, ROWS), shape(ROWS, W), shape(ROWS, W), shape(K, ROWS)),
        (*NEAR_SCRATCH, pltpu.SMEM((1, FL), jnp.int32), pltpu.SemaphoreType.DMA((PD + 2,))),
        limit=48,
    )(
        ids, far_lists, gathered, f_low, field, f_high, q_low, image, q_high,
        local_exp, table, shift_down, down, near_blocks,
    )

    gathered = swap(message, "patch")
    return call(last_step_kernel, [VMEM] * 7, (shape(PD, 2, W),) * 2)(
        pick_column, gathered, alpha, field, image, direction, image1
    )


def solution(mesh):
    return jax.shard_map(
        on_device,
        mesh=mesh,
        in_specs=(
            P("patch", "rhs", None),
            P("patch", None, None, None),
            P("patch", None),
            P("patch", None, None),
            P("patch", None, None),
            P("patch", None),
            P("patch", None, None, None),
            P("patch", None, None),
            P("patch", None, None),
        ),
        out_specs=(P("patch", "rhs", None), P("patch", "rhs", None)),
        check_vma=False,
    )
```

```python
import jax
import jax.numpy as jnp
from jax import lax
from jax.experimental import pallas as pl
from jax.experimental.pallas import tpu as pltpu
from jax.sharding import PartitionSpec as P


HIGH = lax.Precision.HIGH
F32 = jnp.float32
BF16 = jnp.bfloat16
MIB = 1024 * 1024

K = 16
W = 384
E = 64
NB = 4
FL = 4
PD = 8
ROWS = PD * K

SMEM = pl.BlockSpec(memory_space=pltpu.SMEM)
VMEM = pl.BlockSpec(memory_space=pltpu.VMEM)
HBM = pl.BlockSpec(memory_space=pltpu.HBM)


def shape(*dims, dtype=F32):
    return jax.ShapeDtypeStruct(dims, dtype)


def nn(left, right):
    return jnp.dot(left, right, precision=HIGH, preferred_element_type=F32)


def exact(left, right):
    return jnp.dot(left, right, precision=lax.Precision.HIGHEST, preferred_element_type=F32)


def nt(left, right):
    return lax.dot_general(
        left, right, (((1,), (1,)), ((), ())), precision=HIGH, preferred_element_type=F32
    )


def iotas(rows, cols):
    return (
        lax.broadcasted_iota(jnp.int32, (rows, cols), 0),
        lax.broadcasted_iota(jnp.int32, (rows, cols), 1),
    )


def inverse(matrix):
    row, lane = iotas(K, 2 * K)
    eye = jnp.where(lane == row + K, 1.0, 0.0).astype(F32)
    work = jnp.concatenate([matrix, eye[:, K:]], axis=1)
    for i in range(0, K, 2):
        left = jnp.broadcast_to(work[:, i : i + 1], (K, 2 * K))
        right = jnp.broadcast_to(work[:, i + 1 : i + 2], (K, 2 * K))
        a, c = left[i : i + 1], left[i + 1 : i + 2]
        b, d = right[i : i + 1], right[i + 1 : i + 2]
        upper, lower = work[i : i + 1], work[i + 1 : i + 2]
        scale = 1.0 / (a * d - b * c)
        upper, lower = (d * upper - b * lower) * scale, (a * lower - c * upper) * scale
        rest = work - left * upper - right * lower
        work = jnp.where(row == i, upper, jnp.where(row == i + 1, lower, rest))
    return work[:, K:]


def small(left, right):
    terms = [left[:, k : k + 1] * right[k : k + 1, :] for k in range(K)]
    while len(terms) > 1:
        terms = [a + b for a, b in zip(terms[::2], terms[1::2])]
    return terms[0]


def tiled(matrix):
    wide = jnp.concatenate([matrix, jnp.zeros((K, ROWS - K), F32)], axis=1)
    for step in (K, 2 * K, 4 * K):
        wide = wide + pltpu.roll(wide, step, 1)
    return wide


def block_diagonal(matrix):
    wide = jnp.concatenate([tiled(matrix)] * PD, axis=0)
    row, lane = iotas(ROWS, ROWS)
    return jnp.where(row // K == lane // K, wide, 0.0)


def side_by_side(field):
    return jnp.concatenate([field[p * K : (p + 1) * K] for p in range(PD)], axis=1)


def fetch(near_ref, blocks_ref, sems):
    def start(p, carry):
        pltpu.make_async_copy(near_ref.at[p], blocks_ref.at[p], sems.at[p]).start()
        return carry

    lax.fori_loop(0, PD, start, 0)


def fetched(near_ref, blocks_ref, sems):
    def wait(p, carry):
        pltpu.make_async_copy(near_ref.at[p], blocks_ref.at[p], sems.at[p]).wait()
        return carry

    lax.fori_loop(0, PD, wait, 0)


def near_product(ids_ref, blocks_ref, rounded_ref):
    total = None
    for p in range(PD):
        fields = jnp.concatenate([rounded_ref[ids_ref[p, j]] for j in range(NB)], axis=1)
        pieces = [fields]
        if p:
            pieces.insert(0, jnp.zeros((p * K, NB * W), BF16))
        if p + 1 < PD:
            pieces.append(jnp.zeros(((PD - 1 - p) * K, NB * W), BF16))
        fields = jnp.concatenate(pieces, axis=0)
        blocks = jnp.concatenate([blocks_ref[p, j] for j in range(NB)], axis=1)
        part = lax.dot_general(
            blocks, fields, (((1,), (1,)), ((), ())), preferred_element_type=F32
        )
        total = part if total is None else total + part
    return total


def shifted(local_exp, shift_ref):
    return nt(local_exp, shift_ref[...].reshape(PD * E, E))


def far_product(patch_exp, down_ref):
    row, lane = iotas(ROWS, PD * E)
    wide = jnp.concatenate([patch_exp] * PD, axis=0)
    wide = jnp.where(row // K == lane // E, wide, 0.0)
    return nn(wide, down_ref[...].reshape(PD * E, W))


def expansion(chosen, table_ref):
    total = None
    for j in range(FL):
        moment = chosen[j]
        if moment.shape[0] < K:
            moment = jnp.concatenate([moment[:, :E], moment[:, E:]], axis=0)
        part = nt(moment[:, :E], table_ref[j])
        total = part if total is None else total + part
    return total


def summed(parts):
    while len(parts) > 1:
        parts = [a + b for a, b in zip(parts[::2], parts[1::2])]
    return parts[0]


def maps_kernel(up_ref, shift_ref, pick_ref, out_ref, pick_out):
    pick_out[...] = pick_ref[...]
    for p in range(PD):
        out_ref[:, p * W : (p + 1) * W] = nn(shift_ref[p], up_ref[p])


def moment_kernel(field_ref, up_ref, out_ref):
    moment = nt(side_by_side(field_ref[...].reshape(ROWS, W)), up_ref[...])
    message = jnp.concatenate([moment[: K // 2], moment[K // 2 :]], axis=1)
    for i in range(out_ref.shape[0]):
        out_ref[i] = message


def near_kernel(
    ids_ref, low_ref, own_ref, high_ref, near_ref, out_ref, blocks_ref, rounded_ref, ids_smem, sems
):
    ids = pltpu.make_async_copy(ids_ref, ids_smem, sems.at[PD])
    ids.start()
    fetch(near_ref, blocks_ref, sems)
    for i, ref in enumerate((low_ref, own_ref, high_ref)):
        rounded_ref[i * PD : (i + 1) * PD] = ref[...].astype(BF16)
    ids.wait()
    fetched(near_ref, blocks_ref, sems)
    out_ref[...] = near_product(ids_smem, blocks_ref, rounded_ref).T


def image_kernel(
    pick_ref, gathered_ref, near_ref, field_ref, up_ref, table_ref, shift_ref, down_ref,
    image_out, local_out, out_ref,
):
    count = gathered_ref.shape[0]
    chosen = [
        summed([gathered_ref[c] * pick_ref[j * count + c : j * count + c + 1] for c in range(count)])
        for j in range(FL)
    ]
    local_exp = expansion(chosen, table_ref)
    local_out[...] = jnp.concatenate([local_exp, jnp.zeros((K, E), F32)], axis=1)
    image = near_ref[...] + far_product(shifted(local_exp, shift_ref), down_ref)
    image_out[...] = image.reshape(PD, K, W)
    image = side_by_side(image)
    moment = nt(image, up_ref[...])
    both = jnp.concatenate([side_by_side(field_ref[...].reshape(ROWS, W)), image], axis=0)
    grams = nt(both, both)
    message = jnp.concatenate(
        [moment, grams[K:, :], grams[:K, :]], axis=1
    )
    for i in range(out_ref.shape[0]):
        out_ref[i] = message


def total_of(gathered_ref):
    return summed([gathered_ref[i] for i in range(gathered_ref.shape[0])])


def direction_kernel(
    ids_ref, far_ref, gathered_ref, f_low, f_own, f_high, q_low, q_own, q_high,
    local_ref, table_ref, shift_ref, down_ref, near_ref,
    out_ref, direction_out, image_out, alpha_out,
    blocks_ref, rounded_ref, ids_smem, far_smem, sems,
):
    ids = pltpu.make_async_copy(ids_ref, ids_smem, sems.at[PD])
    far_ids = pltpu.make_async_copy(far_ref, far_smem, sems.at[PD + 1])
    ids.start()
    far_ids.start()
    fetch(near_ref, blocks_ref, sems)
    total = total_of(gathered_ref)
    qr = total[:, E : E + K]
    qq = total[:, E + K : E + 2 * K]
    rr = total[:, E + 2 * K : E + 3 * K]
    rq = total[:, E + 3 * K :]
    curve_inv = inverse(0.5 * (qr + rq))
    rr_inv = inverse(rr)
    alpha = small(curve_inv, rr)
    alpha_t = small(rr, curve_inv)
    following = (
        rr - small(rq, alpha) - small(alpha_t, qr) + small(alpha_t, small(qq, alpha))
    )
    row, lane = iotas(K, K)
    lift_t = small(following, rr_inv) + jnp.where(row == lane, 1.0, 0.0)
    alpha_out[...] = jnp.concatenate([alpha_t, jnp.zeros((K, ROWS - K), F32)], axis=1)
    far_ids.wait()
    image_exp = expansion([gathered_ref[far_smem[0, j]] for j in range(FL)], table_ref)
    local_exp = small(lift_t, local_ref[:, :E]) - small(alpha_t, image_exp)
    far = far_product(shifted(local_exp, shift_ref), down_ref)

    coeffs = block_diagonal(-alpha_t)
    both = jnp.concatenate([block_diagonal(lift_t), coeffs], axis=1)
    for i, (f, q) in enumerate(((f_low, q_low), (f_own, q_own), (f_high, q_high))):
        pair = jnp.concatenate(
            [f[...].reshape(ROWS, W), q[...].reshape(ROWS, W)], axis=0
        )
        mixed = exact(both, pair)
        if i == 1:
            direction = mixed
            residual = f_own[...].reshape(ROWS, W) + exact(coeffs, q_own[...].reshape(ROWS, W))
        rounded_ref[i * PD : (i + 1) * PD] = mixed.astype(BF16).reshape(PD, K, W)
    direction_out[...] = direction
    ids.wait()
    fetched(near_ref, blocks_ref, sems)
    image = near_product(ids_smem, blocks_ref, rounded_ref)
    image = image.T + far
    image_out[...] = image
    residual = side_by_side(residual)
    grams = nt(
        jnp.concatenate([side_by_side(image), residual], axis=0),
        jnp.concatenate([side_by_side(direction), residual], axis=0),
    )
    message = jnp.concatenate([grams[:K, :K], grams[K:, K:]], axis=1)
    message = jnp.concatenate(
        [message[: K // 2], message[K // 2 :], jnp.zeros((K // 2, ROWS - 4 * K), F32)], axis=1
    )
    for i in range(out_ref.shape[0]):
        out_ref[i] = message


def own_coeffs(pick, coeffs_t):
    row, lane = iotas(K, ROWS)
    return jnp.where(row // 2 == lane // K, tiled(small(pick, coeffs_t)), 0.0)


def last_step_kernel(
    pick_ref, gathered_ref, alpha_ref, field_ref, image0_ref, direction_ref, image_ref,
    x_out, r_out,
):
    total = total_of(gathered_ref)
    total = jnp.concatenate([total[:, : 2 * K], total[:, 2 * K : 4 * K]], axis=0)
    pick = pick_ref[...]
    qd = total[:, :K]
    field = field_ref[...].reshape(ROWS, W)
    row, lane = iotas(K, ROWS)
    mine = jnp.where(row // 2 == lane // K, tiled(pick), 0.0)
    coeffs0 = own_coeffs(pick, alpha_ref[:, :K])
    x = nn(coeffs0, field)
    r = exact(mine, field) - exact(coeffs0, image0_ref[...].reshape(ROWS, W))
    alpha_t = small(total[:, K : 2 * K], inverse(0.5 * (qd + qd.T)))
    coeffs = own_coeffs(pick, alpha_t)
    x = x + nn(coeffs, direction_ref[...])
    r = r - nn(coeffs, image_ref[...])
    for p in range(PD):
        x_out[p] = x[2 * p : 2 * p + 2]
        r_out[p] = r[2 * p : 2 * p + 2]


def call(kernel, in_specs, out_shape, scratch=(), limit=24, cost=1):
    many = isinstance(out_shape, (tuple, list))
    return pl.pallas_call(
        kernel,
        in_specs=in_specs,
        out_specs=tuple(VMEM for _ in out_shape) if many else VMEM,
        out_shape=out_shape,
        scratch_shapes=scratch,
        compiler_params=pltpu.CompilerParams(vmem_limit_bytes=limit * MIB),
        cost_estimate=pl.CostEstimate(flops=cost * 1_000_000, bytes_accessed=1_000_000, transcendentals=0),
    )


NEAR_SCRATCH = (
    pltpu.VMEM((PD, NB, W, W), BF16),
    pltpu.VMEM((3 * PD, K, W), BF16),
    pltpu.SMEM((PD, NB), jnp.int32),
)


def swap(array, axis):
    return lax.all_to_all(array, axis, 0, 0, tiled=True)


def halo(block, axis):
    count = lax.axis_size(axis)
    forward = [(i, (i + 1) % count) for i in range(count)]
    backward = [(target, source) for source, target in forward]
    return lax.ppermute(block, axis, forward), lax.ppermute(block, axis, backward)


def on_device(
    rhs_vectors,
    near_blocks,
    neighbours,
    up_maps,
    shift_up,
    far_lists,
    translations,
    shift_down,
    down_maps,
):
    count = lax.axis_size("patch")
    depth = lax.axis_size("rhs")
    place = lax.axis_index("rhs").astype(jnp.int32)
    first = lax.axis_index("patch") * PD - PD
    ids = jnp.mod(neighbours - first, PD * count)

    message = jnp.broadcast_to(rhs_vectors[None], (depth, *rhs_vectors.shape))
    parts = swap(message, "rhs")
    field = parts.transpose(1, 2, 0, 3).reshape(PD, K, W)

    row, lane = jnp.arange(K)[:, None], jnp.arange(K)[None, :]
    pick_column = (lane == (row % 2) * PD + place).astype(F32)
    pick_cell = (far_lists[0][:, None] == jnp.arange(count)[None, :]).astype(F32)
    pick_cell = jnp.broadcast_to(pick_cell.reshape(FL * count, 1), (FL * count, 2 * E))

    up, pick_column = call(maps_kernel, [VMEM] * 3, (shape(E, PD * W), shape(K, K)))(
        up_maps, shift_up, pick_column
    )
    table = translations[0]
    down = down_maps.transpose(0, 2, 1)

    f_low, f_high = halo(field, "patch")
    message = call(moment_kernel, [VMEM] * 2, shape(count, K // 2, ROWS))(field, up)
    gathered = swap(message, "patch")
    near = call(
        near_kernel,
        [VMEM] * 4 + [HBM],
        shape(ROWS, W),
        (*NEAR_SCRATCH, pltpu.SemaphoreType.DMA((PD + 1,))),
        limit=48,
    )(
        ids, f_low, field, f_high, near_blocks
    )
    image, local_exp, message = call(
        image_kernel,
        [VMEM] * 8,
        (shape(PD, K, W), shape(K, 2 * E), shape(count, K, ROWS)),
    )(pick_cell, gathered, near, field, up, table, shift_down, down)

    q_low, q_high = halo(image, "patch")
    gathered = swap(message, "patch")
    message, direction, image1, alpha = call(
        direction_kernel,
        [VMEM] * 13 + [HBM],
        (shape(count, K // 2, ROWS), shape(ROWS, W), shape(ROWS, W), shape(K, ROWS)),
        (*NEAR_SCRATCH, pltpu.SMEM((1, FL), jnp.int32), pltpu.SemaphoreType.DMA((PD + 2,))),
        limit=48,
    )(
        ids, far_lists, gathered, f_low, field, f_high, q_low, image, q_high,
        local_exp, table, shift_down, down, near_blocks,
    )

    gathered = swap(message, "patch")
    return call(last_step_kernel, [VMEM] * 7, (shape(PD, 2, W),) * 2)(
        pick_column, gathered, alpha, field, image, direction, image1
    )


def solution(mesh):
    return jax.shard_map(
        on_device,
        mesh=mesh,
        in_specs=(
            P("patch", "rhs", None),
            P("patch", None, None, None),
            P("patch", None),
            P("patch", None, None),
            P("patch", None, None),
            P("patch", None),
            P("patch", None, None, None),
            P("patch", None, None),
            P("patch", None, None),
        ),
        out_specs=(P("patch", "rhs", None), P("patch", "rhs", None)),
        check_vma=False,
    )
```

```python
import jax
import jax.numpy as jnp
from jax import lax
from jax.experimental import pallas as pl
from jax.experimental.pallas import tpu as pltpu
from jax.sharding import PartitionSpec as P


HIGH = lax.Precision.HIGH
F32 = jnp.float32
BF16 = jnp.bfloat16
MIB = 1024 * 1024

K = 16
W = 384
E = 64
NB = 4
FL = 4
PD = 8
ROWS = PD * K

SMEM = pl.BlockSpec(memory_space=pltpu.SMEM)
VMEM = pl.BlockSpec(memory_space=pltpu.VMEM)
HBM = pl.BlockSpec(memory_space=pltpu.HBM)


def shape(*dims, dtype=F32):
    return jax.ShapeDtypeStruct(dims, dtype)


def nn(left, right):
    return jnp.dot(left, right, precision=HIGH, preferred_element_type=F32)


def exact(left, right):
    return jnp.dot(left, right, precision=lax.Precision.HIGHEST, preferred_element_type=F32)


def nt(left, right):
    return lax.dot_general(
        left, right, (((1,), (1,)), ((), ())), precision=HIGH, preferred_element_type=F32
    )


def iotas(rows, cols):
    return (
        lax.broadcasted_iota(jnp.int32, (rows, cols), 0),
        lax.broadcasted_iota(jnp.int32, (rows, cols), 1),
    )


def inverse(matrix):
    row, lane = iotas(K, 2 * K)
    eye = jnp.where(lane == row + K, 1.0, 0.0).astype(F32)
    work = jnp.concatenate([matrix, eye[:, K:]], axis=1)
    for i in range(0, K, 2):
        left = jnp.broadcast_to(work[:, i : i + 1], (K, 2 * K))
        right = jnp.broadcast_to(work[:, i + 1 : i + 2], (K, 2 * K))
        a, c = left[i : i + 1], left[i + 1 : i + 2]
        b, d = right[i : i + 1], right[i + 1 : i + 2]
        upper, lower = work[i : i + 1], work[i + 1 : i + 2]
        scale = 1.0 / (a * d - b * c)
        upper, lower = (d * upper - b * lower) * scale, (a * lower - c * upper) * scale
        rest = work - left * upper - right * lower
        work = jnp.where(row == i, upper, jnp.where(row == i + 1, lower, rest))
    return work[:, K:]


def small(left, right):
    terms = [left[:, k : k + 1] * right[k : k + 1, :] for k in range(K)]
    while len(terms) > 1:
        terms = [a + b for a, b in zip(terms[::2], terms[1::2])]
    return terms[0]


def tiled(matrix):
    wide = jnp.concatenate([matrix, jnp.zeros((K, ROWS - K), F32)], axis=1)
    for step in (K, 2 * K, 4 * K):
        wide = wide + pltpu.roll(wide, step, 1)
    return wide


def block_diagonal(matrix):
    wide = jnp.concatenate([tiled(matrix)] * PD, axis=0)
    row, lane = iotas(ROWS, ROWS)
    return jnp.where(row // K == lane // K, wide, 0.0)


def side_by_side(field):
    return jnp.concatenate([field[p * K : (p + 1) * K] for p in range(PD)], axis=1)


def fetch(near_ref, blocks_ref, sems):
    def start(p, carry):
        pltpu.make_async_copy(near_ref.at[p], blocks_ref.at[p], sems.at[p]).start()
        return carry

    lax.fori_loop(0, PD, start, 0)


def fetched(near_ref, blocks_ref, sems):
    def wait(p, carry):
        pltpu.make_async_copy(near_ref.at[p], blocks_ref.at[p], sems.at[p]).wait()
        return carry

    lax.fori_loop(0, PD, wait, 0)


def near_product(ids_ref, blocks_ref, rounded_ref):
    total = None
    for p in range(PD):
        fields = jnp.concatenate([rounded_ref[ids_ref[p, j]] for j in range(NB)], axis=1)
        pieces = [fields]
        if p:
            pieces.insert(0, jnp.zeros((p * K, NB * W), BF16))
        if p + 1 < PD:
            pieces.append(jnp.zeros(((PD - 1 - p) * K, NB * W), BF16))
        fields = jnp.concatenate(pieces, axis=0)
        blocks = jnp.concatenate([blocks_ref[p, j] for j in range(NB)], axis=1)
        part = lax.dot_general(
            blocks, fields, (((1,), (1,)), ((), ())), preferred_element_type=F32
        )
        total = part if total is None else total + part
    return total


def shifted(local_exp, shift_ref):
    return nt(local_exp, shift_ref[...].reshape(PD * E, E))


def far_product(patch_exp, down_ref):
    row, lane = iotas(ROWS, PD * E)
    wide = jnp.concatenate([patch_exp] * PD, axis=0)
    wide = jnp.where(row // K == lane // E, wide, 0.0)
    return nn(wide, down_ref[...].reshape(PD * E, W))


def expansion(chosen, table_ref):
    total = None
    for j in range(FL):
        moment = chosen[j]
        if moment.shape[0] < K:
            moment = jnp.concatenate([moment[:, :E], moment[:, E:]], axis=0)
        part = nt(moment[:, :E], table_ref[j])
        total = part if total is None else total + part
    return total


def summed(parts):
    while len(parts) > 1:
        parts = [a + b for a, b in zip(parts[::2], parts[1::2])]
    return parts[0]


def maps_kernel(up_ref, shift_ref, pick_ref, out_ref, pick_out):
    pick_out[...] = pick_ref[...]
    for p in range(PD):
        out_ref[:, p * W : (p + 1) * W] = nn(shift_ref[p], up_ref[p])


def moment_kernel(field_ref, up_ref, out_ref):
    moment = nt(side_by_side(field_ref[...].reshape(ROWS, W)), up_ref[...])
    message = jnp.concatenate([moment[: K // 2], moment[K // 2 :]], axis=1)
    for i in range(out_ref.shape[0]):
        out_ref[i] = message


def near_kernel(
    ids_ref, low_ref, own_ref, high_ref, near_ref, out_ref, blocks_ref, rounded_ref, ids_smem, sems
):
    ids = pltpu.make_async_copy(ids_ref, ids_smem, sems.at[PD])
    ids.start()
    fetch(near_ref, blocks_ref, sems)
    for i, ref in enumerate((low_ref, own_ref, high_ref)):
        rounded_ref[i * PD : (i + 1) * PD] = ref[...].astype(BF16)
    ids.wait()
    fetched(near_ref, blocks_ref, sems)
    out_ref[...] = near_product(ids_smem, blocks_ref, rounded_ref).T


def image_kernel(
    pick_ref, gathered_ref, near_ref, field_ref, up_ref, table_ref, shift_ref, down_ref,
    image_out, local_out, out_ref,
):
    count = gathered_ref.shape[0]
    chosen = [
        summed([gathered_ref[c] * pick_ref[j * count + c : j * count + c + 1] for c in range(count)])
        for j in range(FL)
    ]
    local_exp = expansion(chosen, table_ref)
    local_out[...] = jnp.concatenate([local_exp, jnp.zeros((K, E), F32)], axis=1)
    image = near_ref[...] + far_product(shifted(local_exp, shift_ref), down_ref)
    image_out[...] = image.reshape(PD, K, W)
    image = side_by_side(image)
    moment = nt(image, up_ref[...])
    both = jnp.concatenate([side_by_side(field_ref[...].reshape(ROWS, W)), image], axis=0)
    grams = nt(both, both)
    message = jnp.concatenate(
        [moment, grams[K:, :], grams[:K, :]], axis=1
    )
    for i in range(out_ref.shape[0]):
        out_ref[i] = message


def total_of(gathered_ref):
    return summed([gathered_ref[i] for i in range(gathered_ref.shape[0])])


def direction_kernel(
    ids_ref, far_ref, gathered_ref, f_low, f_own, f_high, q_low, q_own, q_high,
    local_ref, table_ref, shift_ref, down_ref, near_ref,
    out_ref, direction_out, image_out, alpha_out,
    blocks_ref, rounded_ref, ids_smem, far_smem, sems,
):
    ids = pltpu.make_async_copy(ids_ref, ids_smem, sems.at[PD])
    far_ids = pltpu.make_async_copy(far_ref, far_smem, sems.at[PD + 1])
    ids.start()
    far_ids.start()
    fetch(near_ref, blocks_ref, sems)
    total = total_of(gathered_ref)
    qr = total[:, E : E + K]
    qq = total[:, E + K : E + 2 * K]
    rr = total[:, E + 2 * K : E + 3 * K]
    rq = total[:, E + 3 * K :]
    curve_inv = inverse(0.5 * (qr + rq))
    rr_inv = inverse(rr)
    alpha = small(curve_inv, rr)
    alpha_t = small(rr, curve_inv)
    following = (
        rr - small(rq, alpha) - small(alpha_t, qr) + small(alpha_t, small(qq, alpha))
    )
    row, lane = iotas(K, K)
    lift_t = small(following, rr_inv) + jnp.where(row == lane, 1.0, 0.0)
    alpha_out[...] = jnp.concatenate([alpha_t, jnp.zeros((K, ROWS - K), F32)], axis=1)
    far_ids.wait()
    image_exp = expansion([gathered_ref[far_smem[0, j]] for j in range(FL)], table_ref)
    local_exp = small(lift_t, local_ref[:, :E]) - small(alpha_t, image_exp)
    far = far_product(shifted(local_exp, shift_ref), down_ref)

    coeffs = block_diagonal(-alpha_t)
    both = jnp.concatenate([block_diagonal(lift_t), coeffs], axis=1)
    for i, (f, q) in enumerate(((f_low, q_low), (f_own, q_own), (f_high, q_high))):
        pair = jnp.concatenate(
            [f[...].reshape(ROWS, W), q[...].reshape(ROWS, W)], axis=0
        )
        mixed = exact(both, pair)
        if i == 1:
            direction = mixed
            residual = f_own[...].reshape(ROWS, W) + exact(coeffs, q_own[...].reshape(ROWS, W))
        rounded_ref[i * PD : (i + 1) * PD] = mixed.astype(BF16).reshape(PD, K, W)
    direction_out[...] = direction
    ids.wait()
    fetched(near_ref, blocks_ref, sems)
    image = near_product(ids_smem, blocks_ref, rounded_ref)
    image = image.T + far
    image_out[...] = image
    residual = side_by_side(residual)
    grams = nt(
        jnp.concatenate([side_by_side(image), residual], axis=0),
        jnp.concatenate([side_by_side(direction), residual], axis=0),
    )
    message = jnp.concatenate([grams[:K, :K], grams[K:, K:]], axis=1)
    message = jnp.concatenate(
        [message[: K // 2], message[K // 2 :], jnp.zeros((K // 2, ROWS - 4 * K), F32)], axis=1
    )
    for i in range(out_ref.shape[0]):
        out_ref[i] = message


def own_coeffs(pick, coeffs_t):
    row, lane = iotas(K, ROWS)
    return jnp.where(row // 2 == lane // K, tiled(small(pick, coeffs_t)), 0.0)


def first_step_kernel(pick_ref, alpha_ref, field_ref, image_ref, x_out, r_out):
    pick = pick_ref[...]
    field = field_ref[...].reshape(ROWS, W)
    row, lane = iotas(K, ROWS)
    mine = jnp.where(row // 2 == lane // K, tiled(pick), 0.0)
    coeffs = own_coeffs(pick, alpha_ref[:, :K])
    x_out[...] = exact(coeffs, field)
    r_out[...] = exact(mine, field) - exact(coeffs, image_ref[...].reshape(ROWS, W))


def last_step_kernel(pick_ref, gathered_ref, direction_ref, image_ref, x_ref, r_ref, x_out, r_out):
    total = total_of(gathered_ref)
    total = jnp.concatenate([total[:, : 2 * K], total[:, 2 * K : 4 * K]], axis=0)
    qd = total[:, :K]
    alpha_t = small(total[:, K : 2 * K], inverse(0.5 * (qd + qd.T)))
    coeffs = own_coeffs(pick_ref[...], alpha_t)
    x = x_ref[...] + nn(coeffs, direction_ref[...])
    r = r_ref[...] - nn(coeffs, image_ref[...])
    for p in range(PD):
        x_out[p] = x[2 * p : 2 * p + 2]
        r_out[p] = r[2 * p : 2 * p + 2]


def call(kernel, in_specs, out_shape, scratch=(), limit=24, cost=1):
    many = isinstance(out_shape, (tuple, list))
    return pl.pallas_call(
        kernel,
        in_specs=in_specs,
        out_specs=tuple(VMEM for _ in out_shape) if many else VMEM,
        out_shape=out_shape,
        scratch_shapes=scratch,
        compiler_params=pltpu.CompilerParams(vmem_limit_bytes=limit * MIB),
        cost_estimate=pl.CostEstimate(flops=cost * 1_000_000, bytes_accessed=1_000_000, transcendentals=0),
    )


NEAR_SCRATCH = (
    pltpu.VMEM((PD, NB, W, W), BF16),
    pltpu.VMEM((3 * PD, K, W), BF16),
    pltpu.SMEM((PD, NB), jnp.int32),
)


def swap(array, axis):
    return lax.all_to_all(array, axis, 0, 0, tiled=True)


def halo(block, axis):
    count = lax.axis_size(axis)
    forward = [(i, (i + 1) % count) for i in range(count)]
    backward = [(target, source) for source, target in forward]
    low = lax.ppermute(block, axis, forward)
    high = lax.ppermute(block, axis, backward)
    return low, high


def on_device(
    rhs_vectors,
    near_blocks,
    neighbours,
    up_maps,
    shift_up,
    far_lists,
    translations,
    shift_down,
    down_maps,
):
    count = lax.axis_size("patch")
    depth = lax.axis_size("rhs")
    place = lax.axis_index("rhs").astype(jnp.int32)
    first = lax.axis_index("patch") * PD - PD
    ids = jnp.mod(neighbours - first, PD * count)

    message = jnp.broadcast_to(rhs_vectors[None], (depth, *rhs_vectors.shape))
    parts = swap(message, "rhs")
    field = parts.transpose(1, 2, 0, 3).reshape(PD, K, W)

    row, lane = jnp.arange(K)[:, None], jnp.arange(K)[None, :]
    pick_column = (lane == (row % 2) * PD + place).astype(F32)
    pick_cell = (far_lists[0][:, None] == jnp.arange(count)[None, :]).astype(F32)
    pick_cell = jnp.broadcast_to(pick_cell.reshape(FL * count, 1), (FL * count, 2 * E))

    up, pick_column = call(maps_kernel, [VMEM] * 3, (shape(E, PD * W), shape(K, K)))(
        up_maps, shift_up, pick_column
    )
    table = translations[0]
    down = down_maps.transpose(0, 2, 1)

    f_low, f_high = halo(field, "patch")
    message = call(moment_kernel, [VMEM] * 2, shape(count, K // 2, ROWS))(field, up)
    gathered = swap(message, "patch")
    near = call(
        near_kernel,
        [VMEM] * 4 + [HBM],
        shape(ROWS, W),
        (*NEAR_SCRATCH, pltpu.SemaphoreType.DMA((PD + 1,))),
        limit=48,
    )(
        ids, f_low, field, f_high, near_blocks
    )
    image, local_exp, message = call(
        image_kernel,
        [VMEM] * 8,
        (shape(PD, K, W), shape(K, 2 * E), shape(count, K, ROWS)),
    )(pick_cell, gathered, near, field, up, table, shift_down, down)

    q_low, q_high = halo(image, "patch")
    gathered = swap(message, "patch")
    message, direction, image1, alpha = call(
        direction_kernel,
        [VMEM] * 13 + [HBM],
        (shape(count, K // 2, ROWS), shape(ROWS, W), shape(ROWS, W), shape(K, ROWS)),
        (*NEAR_SCRATCH, pltpu.SMEM((1, FL), jnp.int32), pltpu.SemaphoreType.DMA((PD + 2,))),
        limit=48,
    )(
        ids, far_lists, gathered, f_low, field, f_high, q_low, image, q_high,
        local_exp, table, shift_down, down, near_blocks,
    )

    gathered = swap(message, "patch")
    x, r = call(first_step_kernel, [VMEM] * 4, (shape(2 * PD, W),) * 2)(
        pick_column, alpha, field, image
    )
    return call(last_step_kernel, [VMEM] * 6, (shape(PD, 2, W),) * 2)(
        pick_column, gathered, direction, image1, x, r
    )


def solution(mesh):
    return jax.shard_map(
        on_device,
        mesh=mesh,
        in_specs=(
            P("patch", "rhs", None),
            P("patch", None, None, None),
            P("patch", None),
            P("patch", None, None),
            P("patch", None, None),
            P("patch", None),
            P("patch", None, None, None),
            P("patch", None, None),
            P("patch", None, None),
        ),
        out_specs=(P("patch", "rhs", None), P("patch", "rhs", None)),
        check_vma=False,
    )
```

```python
import jax
import jax.numpy as jnp
from jax import lax
from jax.experimental import pallas as pl
from jax.experimental.pallas import tpu as pltpu
from jax.sharding import PartitionSpec as P


HIGH = lax.Precision.HIGH
F32 = jnp.float32
BF16 = jnp.bfloat16
MIB = 1024 * 1024

K = 16
W = 384
E = 64
NB = 4
FL = 4
PD = 8
ROWS = PD * K

SMEM = pl.BlockSpec(memory_space=pltpu.SMEM)
VMEM = pl.BlockSpec(memory_space=pltpu.VMEM)
HBM = pl.BlockSpec(memory_space=pltpu.HBM)


def shape(*dims, dtype=F32):
    return jax.ShapeDtypeStruct(dims, dtype)


def nn(left, right):
    return jnp.dot(left, right, precision=HIGH, preferred_element_type=F32)


def exact(left, right):
    return jnp.dot(left, right, precision=lax.Precision.HIGHEST, preferred_element_type=F32)


def nt(left, right):
    return lax.dot_general(
        left, right, (((1,), (1,)), ((), ())), precision=HIGH, preferred_element_type=F32
    )


def iotas(rows, cols):
    return (
        lax.broadcasted_iota(jnp.int32, (rows, cols), 0),
        lax.broadcasted_iota(jnp.int32, (rows, cols), 1),
    )


def inverse(matrix):
    row, lane = iotas(K, 2 * K)
    eye = jnp.where(lane == row + K, 1.0, 0.0).astype(F32)
    work = jnp.concatenate([matrix, eye[:, K:]], axis=1)
    for i in range(0, K, 2):
        left = jnp.broadcast_to(work[:, i : i + 1], (K, 2 * K))
        right = jnp.broadcast_to(work[:, i + 1 : i + 2], (K, 2 * K))
        a, c = left[i : i + 1], left[i + 1 : i + 2]
        b, d = right[i : i + 1], right[i + 1 : i + 2]
        upper, lower = work[i : i + 1], work[i + 1 : i + 2]
        scale = 1.0 / (a * d - b * c)
        upper, lower = (d * upper - b * lower) * scale, (a * lower - c * upper) * scale
        rest = work - left * upper - right * lower
        work = jnp.where(row == i, upper, jnp.where(row == i + 1, lower, rest))
    return work[:, K:]


def small(left, right):
    terms = [left[:, k : k + 1] * right[k : k + 1, :] for k in range(K)]
    while len(terms) > 1:
        terms = [a + b for a, b in zip(terms[::2], terms[1::2])]
    return terms[0]


def tiled(matrix):
    wide = jnp.concatenate([matrix, jnp.zeros((K, ROWS - K), F32)], axis=1)
    for step in (K, 2 * K, 4 * K):
        wide = wide + pltpu.roll(wide, step, 1)
    return wide


def block_diagonal(matrix):
    wide = jnp.concatenate([tiled(matrix)] * PD, axis=0)
    row, lane = iotas(ROWS, ROWS)
    return jnp.where(row // K == lane // K, wide, 0.0)


def side_by_side(field):
    return jnp.concatenate([field[p * K : (p + 1) * K] for p in range(PD)], axis=1)


def fetch(near_ref, blocks_ref, sems):
    def start(p, carry):
        pltpu.make_async_copy(near_ref.at[p], blocks_ref.at[p], sems.at[p]).start()
        return carry

    lax.fori_loop(0, PD, start, 0)


def fetched(near_ref, blocks_ref, sems):
    def wait(p, carry):
        pltpu.make_async_copy(near_ref.at[p], blocks_ref.at[p], sems.at[p]).wait()
        return carry

    lax.fori_loop(0, PD, wait, 0)


def near_product(ids_ref, blocks_ref, rounded_ref):
    total = None
    for p in range(PD):
        fields = jnp.concatenate([rounded_ref[ids_ref[p, j]] for j in range(NB)], axis=1)
        pieces = [fields]
        if p:
            pieces.insert(0, jnp.zeros((p * K, NB * W), BF16))
        if p + 1 < PD:
            pieces.append(jnp.zeros(((PD - 1 - p) * K, NB * W), BF16))
        fields = jnp.concatenate(pieces, axis=0)
        blocks = jnp.concatenate([blocks_ref[p, j] for j in range(NB)], axis=1)
        part = lax.dot_general(
            blocks, fields, (((1,), (1,)), ((), ())), preferred_element_type=F32
        )
        total = part if total is None else total + part
    return total


def shifted(local_exp, shift_ref):
    return nt(local_exp, shift_ref[...].reshape(PD * E, E))


def far_product(patch_exp, down_ref):
    row, lane = iotas(ROWS, PD * E)
    wide = jnp.concatenate([patch_exp] * PD, axis=0)
    wide = jnp.where(row // K == lane // E, wide, 0.0)
    return nn(wide, down_ref[...].reshape(PD * E, W))


def expansion(chosen, table_ref):
    total = None
    for j in range(FL):
        moment = chosen[j]
        if moment.shape[0] < K:
            moment = jnp.concatenate([moment[:, :E], moment[:, E:]], axis=0)
        part = nt(moment[:, :E], table_ref[j])
        total = part if total is None else total + part
    return total


def summed(parts):
    while len(parts) > 1:
        parts = [a + b for a, b in zip(parts[::2], parts[1::2])]
    return parts[0]


def maps_kernel(up_ref, shift_ref, pick_ref, out_ref, pick_out):
    pick_out[...] = pick_ref[...]
    for p in range(PD):
        out_ref[:, p * W : (p + 1) * W] = nn(shift_ref[p], up_ref[p])


def moment_kernel(field_ref, up_ref, out_ref):
    moment = nt(side_by_side(field_ref[...].reshape(ROWS, W)), up_ref[...])
    message = jnp.concatenate([moment[: K // 2], moment[K // 2 :]], axis=1)
    for i in range(out_ref.shape[0]):
        out_ref[i] = message


def near_kernel(
    ids_ref, partner_ref, own_ref, beyond_ref, near_ref, out_ref, blocks_ref, rounded_ref, ids_smem, sems
):
    ids = pltpu.make_async_copy(ids_ref, ids_smem, sems.at[PD])
    ids.start()
    fetch(near_ref, blocks_ref, sems)
    for i, ref in enumerate((partner_ref, own_ref, beyond_ref)):
        rounded_ref[i * PD : (i + 1) * PD] = ref[...].astype(BF16)
    ids.wait()
    fetched(near_ref, blocks_ref, sems)
    out_ref[...] = near_product(ids_smem, blocks_ref, rounded_ref).T


def image_kernel(
    pick_ref, gathered_ref, near_ref, field_ref, up_ref, table_ref, shift_ref, down_ref,
    image_out, local_out, out_ref,
):
    count = gathered_ref.shape[0]
    chosen = [
        summed([gathered_ref[c] * pick_ref[j * count + c : j * count + c + 1] for c in range(count)])
        for j in range(FL)
    ]
    local_exp = expansion(chosen, table_ref)
    local_out[...] = jnp.concatenate([local_exp, jnp.zeros((K, E), F32)], axis=1)
    image = near_ref[...] + far_product(shifted(local_exp, shift_ref), down_ref)
    image_out[...] = image.reshape(PD, K, W)
    image = side_by_side(image)
    moment = nt(image, up_ref[...])
    both = jnp.concatenate([side_by_side(field_ref[...].reshape(ROWS, W)), image], axis=0)
    grams = nt(both, both)
    message = jnp.concatenate(
        [moment, grams[K:, :], grams[:K, :]], axis=1
    )
    for i in range(out_ref.shape[0]):
        out_ref[i] = message


def total_of(gathered_ref):
    return summed([gathered_ref[i] for i in range(gathered_ref.shape[0])])


def direction_kernel(
    ids_ref, far_ref, gathered_ref, f_partner, f_own, f_beyond, q_partner, q_own, q_beyond,
    local_ref, table_ref, shift_ref, down_ref, near_ref,
    out_ref, direction_out, image_out, alpha_out,
    blocks_ref, rounded_ref, ids_smem, far_smem, sems,
):
    ids = pltpu.make_async_copy(ids_ref, ids_smem, sems.at[PD])
    far_ids = pltpu.make_async_copy(far_ref, far_smem, sems.at[PD + 1])
    ids.start()
    far_ids.start()
    fetch(near_ref, blocks_ref, sems)
    total = total_of(gathered_ref)
    qr = total[:, E : E + K]
    qq = total[:, E + K : E + 2 * K]
    rr = total[:, E + 2 * K : E + 3 * K]
    rq = total[:, E + 3 * K :]
    curve_inv = inverse(0.5 * (qr + rq))
    rr_inv = inverse(rr)
    alpha = small(curve_inv, rr)
    alpha_t = small(rr, curve_inv)
    following = (
        rr - small(rq, alpha) - small(alpha_t, qr) + small(alpha_t, small(qq, alpha))
    )
    row, lane = iotas(K, K)
    lift_t = small(following, rr_inv) + jnp.where(row == lane, 1.0, 0.0)
    alpha_out[...] = jnp.concatenate([alpha_t, jnp.zeros((K, ROWS - K), F32)], axis=1)
    far_ids.wait()
    image_exp = expansion([gathered_ref[far_smem[0, j]] for j in range(FL)], table_ref)
    local_exp = small(lift_t, local_ref[:, :E]) - small(alpha_t, image_exp)
    far = far_product(shifted(local_exp, shift_ref), down_ref)

    coeffs = block_diagonal(-alpha_t)
    both = jnp.concatenate([block_diagonal(lift_t), coeffs], axis=1)
    for i, (f, q) in enumerate(((f_partner, q_partner), (f_own, q_own), (f_beyond, q_beyond))):
        pair = jnp.concatenate(
            [f[...].reshape(ROWS, W), q[...].reshape(ROWS, W)], axis=0
        )
        mixed = exact(both, pair)
        if i == 1:
            direction = mixed
            residual = f_own[...].reshape(ROWS, W) + exact(coeffs, q_own[...].reshape(ROWS, W))
        rounded_ref[i * PD : (i + 1) * PD] = mixed.astype(BF16).reshape(PD, K, W)
    direction_out[...] = direction
    ids.wait()
    fetched(near_ref, blocks_ref, sems)
    image = near_product(ids_smem, blocks_ref, rounded_ref)
    image = image.T + far
    image_out[...] = image
    residual = side_by_side(residual)
    grams = nt(
        jnp.concatenate([side_by_side(image), residual], axis=0),
        jnp.concatenate([side_by_side(direction), residual], axis=0),
    )
    message = jnp.concatenate([grams[:K, :K], grams[K:, K:]], axis=1)
    message = jnp.concatenate(
        [message[: K // 2], message[K // 2 :], jnp.zeros((K // 2, ROWS - 4 * K), F32)], axis=1
    )
    for i in range(out_ref.shape[0]):
        out_ref[i] = message


def own_coeffs(pick, coeffs_t):
    row, lane = iotas(K, ROWS)
    return jnp.where(row // 2 == lane // K, tiled(small(pick, coeffs_t)), 0.0)


def first_step_kernel(pick_ref, alpha_ref, field_ref, image_ref, x_out, r_out):
    pick = pick_ref[...]
    field = field_ref[...].reshape(ROWS, W)
    row, lane = iotas(K, ROWS)
    mine = jnp.where(row // 2 == lane // K, tiled(pick), 0.0)
    coeffs = own_coeffs(pick, alpha_ref[:, :K])
    x_out[...] = exact(coeffs, field)
    r_out[...] = exact(mine, field) - exact(coeffs, image_ref[...].reshape(ROWS, W))


def last_step_kernel(pick_ref, gathered_ref, direction_ref, image_ref, x_ref, r_ref, x_out, r_out):
    total = total_of(gathered_ref)
    total = jnp.concatenate([total[:, : 2 * K], total[:, 2 * K : 4 * K]], axis=0)
    qd = total[:, :K]
    alpha_t = small(total[:, K : 2 * K], inverse(0.5 * (qd + qd.T)))
    coeffs = own_coeffs(pick_ref[...], alpha_t)
    x = x_ref[...] + nn(coeffs, direction_ref[...])
    r = r_ref[...] - nn(coeffs, image_ref[...])
    for p in range(PD):
        x_out[p] = x[2 * p : 2 * p + 2]
        r_out[p] = r[2 * p : 2 * p + 2]


def call(kernel, in_specs, out_shape, scratch=(), limit=24, cost=1):
    many = isinstance(out_shape, (tuple, list))
    return pl.pallas_call(
        kernel,
        in_specs=in_specs,
        out_specs=tuple(VMEM for _ in out_shape) if many else VMEM,
        out_shape=out_shape,
        scratch_shapes=scratch,
        compiler_params=pltpu.CompilerParams(vmem_limit_bytes=limit * MIB),
        cost_estimate=pl.CostEstimate(flops=cost * 1_000_000, bytes_accessed=1_000_000, transcendentals=0),
    )


NEAR_SCRATCH = (
    pltpu.VMEM((PD, NB, W, W), BF16),
    pltpu.VMEM((3 * PD, K, W), BF16),
    pltpu.SMEM((PD, NB), jnp.int32),
)


def swap(array, axis):
    return lax.all_to_all(array, axis, 0, 0, tiled=True)


def halo(block, axis):
    count = lax.axis_size(axis)
    partner = lax.ppermute(block, axis, [(i, i ^ 1) for i in range(count)])
    beyond = lax.ppermute(
        block, axis, [(i, (i + (1 if i % 2 else -1)) % count) for i in range(count)]
    )
    return partner, beyond


def on_device(
    rhs_vectors,
    near_blocks,
    neighbours,
    up_maps,
    shift_up,
    far_lists,
    translations,
    shift_down,
    down_maps,
):
    count = lax.axis_size("patch")
    depth = lax.axis_size("rhs")
    place = lax.axis_index("rhs").astype(jnp.int32)
    cell = lax.axis_index("patch")
    owner = neighbours // PD
    slot = jnp.where(owner == cell, 1, jnp.where(owner == cell ^ 1, 0, 2))
    ids = (slot * PD + neighbours % PD).astype(jnp.int32)

    message = jnp.broadcast_to(rhs_vectors[None], (depth, *rhs_vectors.shape))
    parts = swap(message, "rhs")
    field = parts.transpose(1, 2, 0, 3).reshape(PD, K, W)

    row, lane = jnp.arange(K)[:, None], jnp.arange(K)[None, :]
    pick_column = (lane == (row % 2) * PD + place).astype(F32)
    pick_cell = (far_lists[0][:, None] == jnp.arange(count)[None, :]).astype(F32)
    pick_cell = jnp.broadcast_to(pick_cell.reshape(FL * count, 1), (FL * count, 2 * E))

    up, pick_column = call(maps_kernel, [VMEM] * 3, (shape(E, PD * W), shape(K, K)))(
        up_maps, shift_up, pick_column
    )
    table = translations[0]
    down = down_maps.transpose(0, 2, 1)

    f_partner, f_beyond = halo(field, "patch")
    message = call(moment_kernel, [VMEM] * 2, shape(count, K // 2, ROWS))(field, up)
    gathered = swap(message, "patch")
    near = call(
        near_kernel,
        [VMEM] * 4 + [HBM],
        shape(ROWS, W),
        (*NEAR_SCRATCH, pltpu.SemaphoreType.DMA((PD + 1,))),
        limit=48,
    )(
        ids, f_partner, field, f_beyond, near_blocks
    )
    image, local_exp, message = call(
        image_kernel,
        [VMEM] * 8,
        (shape(PD, K, W), shape(K, 2 * E), shape(count, K, ROWS)),
    )(pick_cell, gathered, near, field, up, table, shift_down, down)

    q_partner, q_beyond = halo(image, "patch")
    gathered = swap(message, "patch")
    message, direction, image1, alpha = call(
        direction_kernel,
        [VMEM] * 13 + [HBM],
        (shape(count, K // 2, ROWS), shape(ROWS, W), shape(ROWS, W), shape(K, ROWS)),
        (*NEAR_SCRATCH, pltpu.SMEM((1, FL), jnp.int32), pltpu.SemaphoreType.DMA((PD + 2,))),
        limit=48,
    )(
        ids, far_lists, gathered, f_partner, field, f_beyond, q_partner, image, q_beyond,
        local_exp, table, shift_down, down, near_blocks,
    )

    gathered = swap(message, "patch")
    x, r = call(first_step_kernel, [VMEM] * 4, (shape(2 * PD, W),) * 2)(
        pick_column, alpha, field, image
    )
    return call(last_step_kernel, [VMEM] * 6, (shape(PD, 2, W),) * 2)(
        pick_column, gathered, direction, image1, x, r
    )


def solution(mesh):
    return jax.shard_map(
        on_device,
        mesh=mesh,
        in_specs=(
            P("patch", "rhs", None),
            P("patch", None, None, None),
            P("patch", None),
            P("patch", None, None),
            P("patch", None, None),
            P("patch", None),
            P("patch", None, None, None),
            P("patch", None, None),
            P("patch", None, None),
        ),
        out_specs=(P("patch", "rhs", None), P("patch", "rhs", None)),
        check_vma=False,
    )
```

```python
import jax
import jax.numpy as jnp
from jax import lax
from jax.experimental import pallas as pl
from jax.experimental.pallas import tpu as pltpu
from jax.sharding import PartitionSpec as P


HIGH = lax.Precision.HIGH
F32 = jnp.float32
BF16 = jnp.bfloat16
MIB = 1024 * 1024

K = 16
W = 384
E = 64
NB = 4
FL = 4
PD = 8
ROWS = PD * K

SMEM = pl.BlockSpec(memory_space=pltpu.SMEM)
VMEM = pl.BlockSpec(memory_space=pltpu.VMEM)
HBM = pl.BlockSpec(memory_space=pltpu.HBM)


def shape(*dims, dtype=F32):
    return jax.ShapeDtypeStruct(dims, dtype)


def nn(left, right):
    return jnp.dot(left, right, precision=HIGH, preferred_element_type=F32)


def exact(left, right):
    return jnp.dot(left, right, precision=lax.Precision.HIGHEST, preferred_element_type=F32)


def nt(left, right):
    return lax.dot_general(
        left, right, (((1,), (1,)), ((), ())), precision=HIGH, preferred_element_type=F32
    )


def iotas(rows, cols):
    return (
        lax.broadcasted_iota(jnp.int32, (rows, cols), 0),
        lax.broadcasted_iota(jnp.int32, (rows, cols), 1),
    )


def inverse(matrix):
    row, lane = iotas(K, 2 * K)
    eye = jnp.where(lane == row + K, 1.0, 0.0).astype(F32)
    work = jnp.concatenate([matrix, eye[:, K:]], axis=1)
    for i in range(0, K, 2):
        left = jnp.broadcast_to(work[:, i : i + 1], (K, 2 * K))
        right = jnp.broadcast_to(work[:, i + 1 : i + 2], (K, 2 * K))
        a, c = left[i : i + 1], left[i + 1 : i + 2]
        b, d = right[i : i + 1], right[i + 1 : i + 2]
        upper, lower = work[i : i + 1], work[i + 1 : i + 2]
        scale = 1.0 / (a * d - b * c)
        upper, lower = (d * upper - b * lower) * scale, (a * lower - c * upper) * scale
        rest = work - left * upper - right * lower
        work = jnp.where(row == i, upper, jnp.where(row == i + 1, lower, rest))
    return work[:, K:]


def small(left, right):
    terms = [left[:, k : k + 1] * right[k : k + 1, :] for k in range(K)]
    while len(terms) > 1:
        terms = [a + b for a, b in zip(terms[::2], terms[1::2])]
    return terms[0]


def tiled(matrix):
    wide = jnp.concatenate([matrix, jnp.zeros((K, ROWS - K), F32)], axis=1)
    for step in (K, 2 * K, 4 * K):
        wide = wide + pltpu.roll(wide, step, 1)
    return wide


def block_diagonal(matrix):
    wide = jnp.concatenate([tiled(matrix)] * PD, axis=0)
    row, lane = iotas(ROWS, ROWS)
    return jnp.where(row // K == lane // K, wide, 0.0)


def side_by_side(field):
    return jnp.concatenate([field[p * K : (p + 1) * K] for p in range(PD)], axis=1)


def fetch(near_ref, blocks_ref, sems):
    def start(p, carry):
        pltpu.make_async_copy(near_ref.at[p], blocks_ref.at[p], sems.at[p]).start()
        return carry

    lax.fori_loop(0, PD, start, 0)


def fetched(near_ref, blocks_ref, sems):
    def wait(p, carry):
        pltpu.make_async_copy(near_ref.at[p], blocks_ref.at[p], sems.at[p]).wait()
        return carry

    lax.fori_loop(0, PD, wait, 0)


def near_product(ids_ref, blocks_ref, rounded_ref):
    total = None
    for p in range(PD):
        fields = jnp.concatenate([rounded_ref[ids_ref[p, j]] for j in range(NB)], axis=1)
        pieces = [fields]
        if p:
            pieces.insert(0, jnp.zeros((p * K, NB * W), BF16))
        if p + 1 < PD:
            pieces.append(jnp.zeros(((PD - 1 - p) * K, NB * W), BF16))
        fields = jnp.concatenate(pieces, axis=0)
        blocks = jnp.concatenate([blocks_ref[p, j] for j in range(NB)], axis=1)
        part = lax.dot_general(
            blocks, fields, (((1,), (1,)), ((), ())), preferred_element_type=F32
        )
        total = part if total is None else total + part
    return total


def shifted(local_exp, shift_ref):
    return nt(local_exp, shift_ref[...].reshape(PD * E, E))


def far_product(patch_exp, down_ref):
    row, lane = iotas(ROWS, PD * E)
    wide = jnp.concatenate([patch_exp] * PD, axis=0)
    wide = jnp.where(row // K == lane // E, wide, 0.0)
    return nn(wide, down_ref[...].reshape(PD * E, W))


def expansion(chosen, table_ref):
    total = None
    for j in range(FL):
        moment = chosen[j]
        if moment.shape[0] < K:
            moment = jnp.concatenate([moment[:, :E], moment[:, E:]], axis=0)
        part = nt(moment[:, :E], table_ref[j])
        total = part if total is None else total + part
    return total


def summed(parts):
    while len(parts) > 1:
        parts = [a + b for a, b in zip(parts[::2], parts[1::2])]
    return parts[0]


def maps_kernel(up_ref, shift_ref, pick_ref, out_ref, pick_out):
    pick_out[...] = pick_ref[...]
    for p in range(PD):
        out_ref[:, p * W : (p + 1) * W] = nn(shift_ref[p], up_ref[p])


def moment_kernel(field_ref, up_ref, out_ref):
    moment = nt(side_by_side(field_ref[...].reshape(ROWS, W)), up_ref[...])
    message = jnp.concatenate([moment[: K // 2], moment[K // 2 :]], axis=1)
    for i in range(out_ref.shape[0]):
        out_ref[i] = message


def near_kernel(
    ids_ref, partner_ref, own_ref, beyond_ref, near_ref, out_ref, blocks_ref, rounded_ref, ids_smem, sems
):
    ids = pltpu.make_async_copy(ids_ref, ids_smem, sems.at[PD])
    ids.start()
    fetch(near_ref, blocks_ref, sems)
    for i, ref in enumerate((partner_ref, own_ref, beyond_ref)):
        rounded_ref[i * PD : (i + 1) * PD] = ref[...].astype(BF16)
    ids.wait()
    fetched(near_ref, blocks_ref, sems)
    out_ref[...] = near_product(ids_smem, blocks_ref, rounded_ref).T


def image_kernel(
    pick_ref, gathered_ref, near_ref, field_ref, up_ref, table_ref, shift_ref, down_ref,
    image_out, local_out, out_ref,
):
    count = gathered_ref.shape[0]
    chosen = [
        summed([gathered_ref[c] * pick_ref[j * count + c : j * count + c + 1] for c in range(count)])
        for j in range(FL)
    ]
    local_exp = expansion(chosen, table_ref)
    local_out[...] = jnp.concatenate([local_exp, jnp.zeros((K, E), F32)], axis=1)
    image = near_ref[...] + far_product(shifted(local_exp, shift_ref), down_ref)
    image_out[...] = image.reshape(PD, K, W)
    image = side_by_side(image)
    moment = nt(image, up_ref[...])
    both = jnp.concatenate([side_by_side(field_ref[...].reshape(ROWS, W)), image], axis=0)
    grams = nt(both, both)
    message = jnp.concatenate(
        [moment, grams[K:, :], grams[:K, :]], axis=1
    )
    for i in range(out_ref.shape[0]):
        out_ref[i] = message


def total_of(gathered_ref):
    return summed([gathered_ref[i] for i in range(gathered_ref.shape[0])])


def direction_kernel(
    ids_ref, far_ref, gathered_ref, f_partner, f_own, f_beyond, q_partner, q_own, q_beyond,
    local_ref, table_ref, shift_ref, down_ref, near_ref,
    out_ref, direction_out, image_out, alpha_out,
    blocks_ref, rounded_ref, ids_smem, far_smem, sems,
):
    ids = pltpu.make_async_copy(ids_ref, ids_smem, sems.at[PD])
    far_ids = pltpu.make_async_copy(far_ref, far_smem, sems.at[PD + 1])
    ids.start()
    far_ids.start()
    fetch(near_ref, blocks_ref, sems)
    total = total_of(gathered_ref)
    qr = total[:, E : E + K]
    qq = total[:, E + K : E + 2 * K]
    rr = total[:, E + 2 * K : E + 3 * K]
    rq = total[:, E + 3 * K :]
    curve_inv = inverse(0.5 * (qr + rq))
    rr_inv = inverse(rr)
    alpha = small(curve_inv, rr)
    alpha_t = small(rr, curve_inv)
    following = (
        rr - small(rq, alpha) - small(alpha_t, qr) + small(alpha_t, small(qq, alpha))
    )
    row, lane = iotas(K, K)
    lift_t = small(following, rr_inv) + jnp.where(row == lane, 1.0, 0.0)
    alpha_out[...] = jnp.concatenate([alpha_t, jnp.zeros((K, ROWS - K), F32)], axis=1)
    far_ids.wait()
    image_exp = expansion([gathered_ref[far_smem[0, j]] for j in range(FL)], table_ref)
    local_exp = small(lift_t, local_ref[:, :E]) - small(alpha_t, image_exp)
    far = far_product(shifted(local_exp, shift_ref), down_ref)

    coeffs = block_diagonal(-alpha_t)
    both = jnp.concatenate([block_diagonal(lift_t), coeffs], axis=1)
    for i, (f, q) in enumerate(((f_partner, q_partner), (f_own, q_own), (f_beyond, q_beyond))):
        pair = jnp.concatenate(
            [f[...].reshape(ROWS, W), q[...].reshape(ROWS, W)], axis=0
        )
        mixed = exact(both, pair)
        if i == 1:
            direction = mixed
            residual = f_own[...].reshape(ROWS, W) + exact(coeffs, q_own[...].reshape(ROWS, W))
        rounded_ref[i * PD : (i + 1) * PD] = mixed.astype(BF16).reshape(PD, K, W)
    direction_out[...] = direction
    ids.wait()
    fetched(near_ref, blocks_ref, sems)
    image = near_product(ids_smem, blocks_ref, rounded_ref)
    image = image.T + far
    image_out[...] = image
    residual = side_by_side(residual)
    image = side_by_side(image)
    direction = side_by_side(direction)
    both = jnp.concatenate([image, residual], axis=0)
    grams = nt(both, jnp.concatenate([direction, residual], axis=0))
    message = jnp.concatenate([grams[:K, :K], nt(direction, image), grams[K:, K:]], axis=1)
    message = jnp.concatenate(
        [message[: K // 2], message[K // 2 :], jnp.zeros((K // 2, ROWS - 6 * K), F32)], axis=1
    )
    for i in range(out_ref.shape[0]):
        out_ref[i] = message


def own_coeffs(rows):
    row, lane = iotas(K, ROWS)
    return jnp.where(row // 2 == lane // K, tiled(rows), 0.0)


def first_step_kernel(pick_ref, alpha_ref, field_ref, image_ref, x_out, r_out):
    pick = pick_ref[...]
    field = field_ref[...].reshape(ROWS, W)
    mine = own_coeffs(pick)
    coeffs = own_coeffs(small(pick, alpha_ref[:, :K]))
    x_out[...] = exact(coeffs, field)
    r_out[...] = exact(mine, field) - exact(coeffs, image_ref[...].reshape(ROWS, W))


def last_step_kernel(pick_ref, gathered_ref, direction_ref, image_ref, x_ref, r_ref, x_out, r_out):
    total = total_of(gathered_ref)
    total = jnp.concatenate([total[:, : 3 * K], total[:, 3 * K : 6 * K]], axis=0)
    mine = small(pick_ref[...], total[:, 2 * K :])
    coeffs = own_coeffs(small(mine, inverse(0.5 * (total[:, :K] + total[:, K : 2 * K]))))
    x = x_ref[...] + nn(coeffs, direction_ref[...])
    r = r_ref[...] - nn(coeffs, image_ref[...])
    for p in range(PD):
        x_out[p] = x[2 * p : 2 * p + 2]
        r_out[p] = r[2 * p : 2 * p + 2]


def call(kernel, in_specs, out_shape, scratch=(), limit=24, cost=1):
    many = isinstance(out_shape, (tuple, list))
    return pl.pallas_call(
        kernel,
        in_specs=in_specs,
        out_specs=tuple(VMEM for _ in out_shape) if many else VMEM,
        out_shape=out_shape,
        scratch_shapes=scratch,
        compiler_params=pltpu.CompilerParams(vmem_limit_bytes=limit * MIB),
        cost_estimate=pl.CostEstimate(flops=cost * 1_000_000, bytes_accessed=1_000_000, transcendentals=0),
    )


NEAR_SCRATCH = (
    pltpu.VMEM((PD, NB, W, W), BF16),
    pltpu.VMEM((3 * PD, K, W), BF16),
    pltpu.SMEM((PD, NB), jnp.int32),
)


def swap(array, axis):
    return lax.all_to_all(array, axis, 0, 0, tiled=True)


def halo(block, axis):
    count = lax.axis_size(axis)
    partner = lax.ppermute(block, axis, [(i, i ^ 1) for i in range(count)])
    beyond = lax.ppermute(
        block, axis, [(i, (i + (1 if i % 2 else -1)) % count) for i in range(count)]
    )
    return partner, beyond


def on_device(
    rhs_vectors,
    near_blocks,
    neighbours,
    up_maps,
    shift_up,
    far_lists,
    translations,
    shift_down,
    down_maps,
):
    count = lax.axis_size("patch")
    depth = lax.axis_size("rhs")
    place = lax.axis_index("rhs").astype(jnp.int32)
    cell = lax.axis_index("patch")
    owner = neighbours // PD
    slot = jnp.where(owner == cell, 1, jnp.where(owner == cell ^ 1, 0, 2))
    ids = (slot * PD + neighbours % PD).astype(jnp.int32)

    message = jnp.broadcast_to(rhs_vectors[None], (depth, *rhs_vectors.shape))
    parts = swap(message, "rhs")
    field = parts.transpose(1, 2, 0, 3).reshape(PD, K, W)

    row, lane = jnp.arange(K)[:, None], jnp.arange(K)[None, :]
    pick_column = (lane == (row % 2) * PD + place).astype(F32)
    pick_cell = (far_lists[0][:, None] == jnp.arange(count)[None, :]).astype(F32)
    pick_cell = jnp.broadcast_to(pick_cell.reshape(FL * count, 1), (FL * count, 2 * E))

    up, pick_column = call(maps_kernel, [VMEM] * 3, (shape(E, PD * W), shape(K, K)))(
        up_maps, shift_up, pick_column
    )
    table = translations[0]
    down = down_maps.transpose(0, 2, 1)

    f_partner, f_beyond = halo(field, "patch")
    message = call(moment_kernel, [VMEM] * 2, shape(count, K // 2, ROWS))(field, up)
    gathered = swap(message, "patch")
    near = call(
        near_kernel,
        [VMEM] * 4 + [HBM],
        shape(ROWS, W),
        (*NEAR_SCRATCH, pltpu.SemaphoreType.DMA((PD + 1,))),
        limit=48,
    )(
        ids, f_partner, field, f_beyond, near_blocks
    )
    image, local_exp, message = call(
        image_kernel,
        [VMEM] * 8,
        (shape(PD, K, W), shape(K, 2 * E), shape(count, K, ROWS)),
    )(pick_cell, gathered, near, field, up, table, shift_down, down)

    q_partner, q_beyond = halo(image, "patch")
    gathered = swap(message, "patch")
    message, direction, image1, alpha = call(
        direction_kernel,
        [VMEM] * 13 + [HBM],
        (shape(count, K // 2, ROWS), shape(ROWS, W), shape(ROWS, W), shape(K, ROWS)),
        (*NEAR_SCRATCH, pltpu.SMEM((1, FL), jnp.int32), pltpu.SemaphoreType.DMA((PD + 2,))),
        limit=48,
    )(
        ids, far_lists, gathered, f_partner, field, f_beyond, q_partner, image, q_beyond,
        local_exp, table, shift_down, down, near_blocks,
    )

    gathered = swap(message, "patch")
    x, r = call(first_step_kernel, [VMEM] * 4, (shape(2 * PD, W),) * 2)(
        pick_column, alpha, field, image
    )
    return call(last_step_kernel, [VMEM] * 6, (shape(PD, 2, W),) * 2)(
        pick_column, gathered, direction, image1, x, r
    )


def solution(mesh):
    return jax.shard_map(
        on_device,
        mesh=mesh,
        in_specs=(
            P("patch", "rhs", None),
            P("patch", None, None, None),
            P("patch", None),
            P("patch", None, None),
            P("patch", None, None),
            P("patch", None),
            P("patch", None, None, None),
            P("patch", None, None),
            P("patch", None, None),
        ),
        out_specs=(P("patch", "rhs", None), P("patch", "rhs", None)),
        check_vma=False,
    )
```

```python
import jax
import jax.numpy as jnp
from jax import lax
from jax.experimental import pallas as pl
from jax.experimental.pallas import tpu as pltpu
from jax.sharding import PartitionSpec as P


HIGH = lax.Precision.HIGH
F32 = jnp.float32
BF16 = jnp.bfloat16
MIB = 1024 * 1024

K = 16
W = 384
E = 64
NB = 4
FL = 4
PD = 8
ROWS = PD * K

SMEM = pl.BlockSpec(memory_space=pltpu.SMEM)
VMEM = pl.BlockSpec(memory_space=pltpu.VMEM)
HBM = pl.BlockSpec(memory_space=pltpu.HBM)


def shape(*dims, dtype=F32):
    return jax.ShapeDtypeStruct(dims, dtype)


def nn(left, right):
    return jnp.dot(left, right, precision=HIGH, preferred_element_type=F32)


def exact(left, right):
    return jnp.dot(left, right, precision=lax.Precision.HIGHEST, preferred_element_type=F32)


def nt(left, right):
    return lax.dot_general(
        left, right, (((1,), (1,)), ((), ())), precision=HIGH, preferred_element_type=F32
    )


def iotas(rows, cols):
    return (
        lax.broadcasted_iota(jnp.int32, (rows, cols), 0),
        lax.broadcasted_iota(jnp.int32, (rows, cols), 1),
    )


def inverse(matrix):
    row, lane = iotas(K, 2 * K)
    eye = jnp.where(lane == row + K, 1.0, 0.0).astype(F32)
    work = jnp.concatenate([matrix, eye[:, K:]], axis=1)
    for i in range(0, K, 2):
        left = jnp.broadcast_to(work[:, i : i + 1], (K, 2 * K))
        right = jnp.broadcast_to(work[:, i + 1 : i + 2], (K, 2 * K))
        a, c = left[i : i + 1], left[i + 1 : i + 2]
        b, d = right[i : i + 1], right[i + 1 : i + 2]
        upper, lower = work[i : i + 1], work[i + 1 : i + 2]
        scale = 1.0 / (a * d - b * c)
        upper, lower = (d * upper - b * lower) * scale, (a * lower - c * upper) * scale
        rest = work - left * upper - right * lower
        work = jnp.where(row == i, upper, jnp.where(row == i + 1, lower, rest))
    return work[:, K:]


def small(left, right):
    terms = [left[:, k : k + 1] * right[k : k + 1, :] for k in range(K)]
    while len(terms) > 1:
        terms = [a + b for a, b in zip(terms[::2], terms[1::2])]
    return terms[0]


def tiled(matrix):
    wide = jnp.concatenate([matrix, jnp.zeros((K, ROWS - K), F32)], axis=1)
    for step in (K, 2 * K, 4 * K):
        wide = wide + pltpu.roll(wide, step, 1)
    return wide


def block_diagonal(matrix):
    wide = jnp.concatenate([tiled(matrix)] * PD, axis=0)
    row, lane = iotas(ROWS, ROWS)
    return jnp.where(row // K == lane // K, wide, 0.0)


def side_by_side(field):
    return jnp.concatenate([field[p * K : (p + 1) * K] for p in range(PD)], axis=1)


def fetch(near_ref, blocks_ref, sems):
    def start(p, carry):
        pltpu.make_async_copy(near_ref.at[p], blocks_ref.at[p], sems.at[p]).start()
        return carry

    lax.fori_loop(0, PD, start, 0)


def fetched(near_ref, blocks_ref, sems):
    def wait(p, carry):
        pltpu.make_async_copy(near_ref.at[p], blocks_ref.at[p], sems.at[p]).wait()
        return carry

    lax.fori_loop(0, PD, wait, 0)


def near_product(ids_ref, blocks_ref, rounded_ref):
    total = None
    for p in range(PD):
        fields = jnp.concatenate([rounded_ref[ids_ref[p, j]] for j in range(NB)], axis=1)
        pieces = [fields]
        if p:
            pieces.insert(0, jnp.zeros((p * K, NB * W), BF16))
        if p + 1 < PD:
            pieces.append(jnp.zeros(((PD - 1 - p) * K, NB * W), BF16))
        fields = jnp.concatenate(pieces, axis=0)
        blocks = jnp.concatenate([blocks_ref[p, j] for j in range(NB)], axis=1)
        part = lax.dot_general(
            blocks, fields, (((1,), (1,)), ((), ())), preferred_element_type=F32
        )
        total = part if total is None else total + part
    return total


def shifted(local_exp, shift_ref):
    return nt(local_exp, shift_ref[...].reshape(PD * E, E))


def far_product(patch_exp, down_ref):
    row, lane = iotas(ROWS, PD * E)
    wide = jnp.concatenate([patch_exp] * PD, axis=0)
    wide = jnp.where(row // K == lane // E, wide, 0.0)
    return nn(wide, down_ref[...].reshape(PD * E, W))


def expansion(chosen, table_ref):
    total = None
    for j in range(FL):
        moment = chosen[j]
        if moment.shape[0] < K:
            moment = jnp.concatenate([moment[:, :E], moment[:, E:]], axis=0)
        part = nt(moment[:, :E], table_ref[j])
        total = part if total is None else total + part
    return total


def summed(parts):
    while len(parts) > 1:
        parts = [a + b for a, b in zip(parts[::2], parts[1::2])]
    return parts[0]


def maps_kernel(up_ref, shift_ref, pick_ref, out_ref, pick_out):
    pick_out[...] = pick_ref[...]
    for p in range(PD):
        out_ref[:, p * W : (p + 1) * W] = nn(shift_ref[p], up_ref[p])


def moment_kernel(field_ref, up_ref, out_ref):
    moment = nt(side_by_side(field_ref[...].reshape(ROWS, W)), up_ref[...])
    message = jnp.concatenate([moment[: K // 2], moment[K // 2 :]], axis=1)
    for i in range(out_ref.shape[0]):
        out_ref[i] = message


def near_kernel(
    ids_ref, partner_ref, own_ref, beyond_ref, near_ref, out_ref, blocks_ref, rounded_ref, ids_smem, sems
):
    ids = pltpu.make_async_copy(ids_ref, ids_smem, sems.at[PD])
    ids.start()
    fetch(near_ref, blocks_ref, sems)
    for i, ref in enumerate((partner_ref, own_ref, beyond_ref)):
        rounded_ref[i * PD : (i + 1) * PD] = ref[...].astype(BF16)
    ids.wait()
    fetched(near_ref, blocks_ref, sems)
    out_ref[...] = near_product(ids_smem, blocks_ref, rounded_ref).T


def image_kernel(
    pick_ref, gathered_ref, near_ref, field_ref, up_ref, table_ref, shift_ref, down_ref,
    image_out, local_out, out_ref,
):
    count = gathered_ref.shape[0]
    chosen = [
        summed([gathered_ref[c] * pick_ref[j * count + c : j * count + c + 1] for c in range(count)])
        for j in range(FL)
    ]
    local_exp = expansion(chosen, table_ref)
    local_out[...] = jnp.concatenate([local_exp, jnp.zeros((K, E), F32)], axis=1)
    image = near_ref[...] + far_product(shifted(local_exp, shift_ref), down_ref)
    image_out[...] = image.reshape(PD, K, W)
    image = side_by_side(image)
    moment = nt(image, up_ref[...])
    both = jnp.concatenate([side_by_side(field_ref[...].reshape(ROWS, W)), image], axis=0)
    grams = nt(both, both)
    message = jnp.concatenate(
        [moment, grams[K:, :], grams[:K, :]], axis=1
    )
    for i in range(out_ref.shape[0]):
        out_ref[i] = message


def total_of(gathered_ref):
    return summed([gathered_ref[i] for i in range(gathered_ref.shape[0])])


def direction_kernel(
    ids_ref, far_ref, gathered_ref, f_partner, f_own, f_beyond, q_partner, q_own, q_beyond,
    local_ref, table_ref, shift_ref, down_ref, near_ref,
    out_ref, direction_out, image_out, alpha_out,
    blocks_ref, rounded_ref, ids_smem, far_smem, sems,
):
    ids = pltpu.make_async_copy(ids_ref, ids_smem, sems.at[PD])
    far_ids = pltpu.make_async_copy(far_ref, far_smem, sems.at[PD + 1])
    ids.start()
    far_ids.start()
    fetch(near_ref, blocks_ref, sems)
    total = total_of(gathered_ref)
    qr = total[:, E : E + K]
    qq = total[:, E + K : E + 2 * K]
    rr = total[:, E + 2 * K : E + 3 * K]
    rq = total[:, E + 3 * K :]
    curve_inv = inverse(0.5 * (qr + rq))
    rr_inv = inverse(rr)
    alpha = small(curve_inv, rr)
    alpha_t = small(rr, curve_inv)
    following = (
        rr - small(rq, alpha) - small(alpha_t, qr) + small(alpha_t, small(qq, alpha))
    )
    row, lane = iotas(K, K)
    lift_t = small(following, rr_inv) + jnp.where(row == lane, 1.0, 0.0)
    alpha_out[...] = jnp.concatenate([alpha_t, jnp.zeros((K, ROWS - K), F32)], axis=1)
    far_ids.wait()
    image_exp = expansion([gathered_ref[far_smem[0, j]] for j in range(FL)], table_ref)
    local_exp = small(lift_t, local_ref[:, :E]) - small(alpha_t, image_exp)
    far = far_product(shifted(local_exp, shift_ref), down_ref)

    coeffs = block_diagonal(-alpha_t)
    both = jnp.concatenate([block_diagonal(lift_t), coeffs], axis=1)
    for i, (f, q) in enumerate(((f_partner, q_partner), (f_own, q_own), (f_beyond, q_beyond))):
        pair = jnp.concatenate(
            [f[...].reshape(ROWS, W), q[...].reshape(ROWS, W)], axis=0
        )
        mixed = exact(both, pair)
        if i == 1:
            direction = mixed
            residual = f_own[...].reshape(ROWS, W) + exact(coeffs, q_own[...].reshape(ROWS, W))
        rounded_ref[i * PD : (i + 1) * PD] = mixed.astype(BF16).reshape(PD, K, W)
    direction_out[...] = direction
    ids.wait()
    fetched(near_ref, blocks_ref, sems)
    image = near_product(ids_smem, blocks_ref, rounded_ref)
    image = image.T + far
    image_out[...] = image
    residual = side_by_side(residual)
    grams = nt(
        jnp.concatenate([side_by_side(image), residual], axis=0),
        jnp.concatenate([side_by_side(direction), residual], axis=0),
    )
    message = jnp.concatenate([grams[:K, :K], grams[K:, K:]], axis=1)
    message = jnp.concatenate(
        [message[: K // 2], message[K // 2 :], jnp.zeros((K // 2, ROWS - 4 * K), F32)], axis=1
    )
    for i in range(out_ref.shape[0]):
        out_ref[i] = message


def own_coeffs(pick, coeffs_t):
    row, lane = iotas(K, ROWS)
    return jnp.where(row // 2 == lane // K, tiled(small(pick, coeffs_t)), 0.0)


def last_step_kernel(
    pick_ref, gathered_ref, alpha_ref, field_ref, image0_ref, direction_ref, image_ref,
    x_out, r_out,
):
    pick = pick_ref[...]
    field = field_ref[...].reshape(ROWS, W)
    row, lane = iotas(K, ROWS)
    mine = jnp.where(row // 2 == lane // K, tiled(pick), 0.0)
    coeffs0 = own_coeffs(pick, alpha_ref[:, :K])
    x = exact(coeffs0, field)
    r = exact(mine, field) - exact(coeffs0, image0_ref[...].reshape(ROWS, W))
    total = total_of(gathered_ref)
    total = jnp.concatenate([total[:, : 2 * K], total[:, 2 * K : 4 * K]], axis=0)
    qd = total[:, :K]
    alpha_t = small(total[:, K : 2 * K], inverse(0.5 * (qd + qd.T)))
    coeffs = own_coeffs(pick, alpha_t)
    x = x + nn(coeffs, direction_ref[...])
    r = r - nn(coeffs, image_ref[...])
    for p in range(PD):
        x_out[p] = x[2 * p : 2 * p + 2]
        r_out[p] = r[2 * p : 2 * p + 2]


def call(kernel, in_specs, out_shape, scratch=(), limit=24, cost=1):
    many = isinstance(out_shape, (tuple, list))
    return pl.pallas_call(
        kernel,
        in_specs=in_specs,
        out_specs=tuple(VMEM for _ in out_shape) if many else VMEM,
        out_shape=out_shape,
        scratch_shapes=scratch,
        compiler_params=pltpu.CompilerParams(vmem_limit_bytes=limit * MIB),
        cost_estimate=pl.CostEstimate(flops=cost * 1_000_000, bytes_accessed=1_000_000, transcendentals=0),
    )


NEAR_SCRATCH = (
    pltpu.VMEM((PD, NB, W, W), BF16),
    pltpu.VMEM((3 * PD, K, W), BF16),
    pltpu.SMEM((PD, NB), jnp.int32),
)


def swap(array, axis):
    return lax.all_to_all(array, axis, 0, 0, tiled=True)


def halo(block, axis):
    count = lax.axis_size(axis)
    partner = lax.ppermute(block, axis, [(i, i ^ 1) for i in range(count)])
    beyond = lax.ppermute(
        block, axis, [(i, (i + (1 if i % 2 else -1)) % count) for i in range(count)]
    )
    return partner, beyond


def on_device(
    rhs_vectors,
    near_blocks,
    neighbours,
    up_maps,
    shift_up,
    far_lists,
    translations,
    shift_down,
    down_maps,
):
    count = lax.axis_size("patch")
    depth = lax.axis_size("rhs")
    place = lax.axis_index("rhs").astype(jnp.int32)
    cell = lax.axis_index("patch")
    owner = neighbours // PD
    slot = jnp.where(owner == cell, 1, jnp.where(owner == cell ^ 1, 0, 2))
    ids = (slot * PD + neighbours % PD).astype(jnp.int32)

    message = jnp.broadcast_to(rhs_vectors[None], (depth, *rhs_vectors.shape))
    parts = swap(message, "rhs")
    field = parts.transpose(1, 2, 0, 3).reshape(PD, K, W)

    row, lane = jnp.arange(K)[:, None], jnp.arange(K)[None, :]
    pick_column = (lane == (row % 2) * PD + place).astype(F32)
    pick_cell = (far_lists[0][:, None] == jnp.arange(count)[None, :]).astype(F32)
    pick_cell = jnp.broadcast_to(pick_cell.reshape(FL * count, 1), (FL * count, 2 * E))

    up, pick_column = call(maps_kernel, [VMEM] * 3, (shape(E, PD * W), shape(K, K)))(
        up_maps, shift_up, pick_column
    )
    table = translations[0]
    down = down_maps.transpose(0, 2, 1)

    f_partner, f_beyond = halo(field, "patch")
    message = call(moment_kernel, [VMEM] * 2, shape(count, K // 2, ROWS))(field, up)
    gathered = swap(message, "patch")
    near = call(
        near_kernel,
        [VMEM] * 4 + [HBM],
        shape(ROWS, W),
        (*NEAR_SCRATCH, pltpu.SemaphoreType.DMA((PD + 1,))),
        limit=48,
    )(
        ids, f_partner, field, f_beyond, near_blocks
    )
    image, local_exp, message = call(
        image_kernel,
        [VMEM] * 8,
        (shape(PD, K, W), shape(K, 2 * E), shape(count, K, ROWS)),
    )(pick_cell, gathered, near, field, up, table, shift_down, down)

    q_partner, q_beyond = halo(image, "patch")
    gathered = swap(message, "patch")
    message, direction, image1, alpha = call(
        direction_kernel,
        [VMEM] * 13 + [HBM],
        (shape(count, K // 2, ROWS), shape(ROWS, W), shape(ROWS, W), shape(K, ROWS)),
        (*NEAR_SCRATCH, pltpu.SMEM((1, FL), jnp.int32), pltpu.SemaphoreType.DMA((PD + 2,))),
        limit=48,
    )(
        ids, far_lists, gathered, f_partner, field, f_beyond, q_partner, image, q_beyond,
        local_exp, table, shift_down, down, near_blocks,
    )

    gathered = swap(message, "patch")
    return call(last_step_kernel, [VMEM] * 7, (shape(PD, 2, W),) * 2)(
        pick_column, gathered, alpha, field, image, direction, image1
    )


def solution(mesh):
    return jax.shard_map(
        on_device,
        mesh=mesh,
        in_specs=(
            P("patch", "rhs", None),
            P("patch", None, None, None),
            P("patch", None),
            P("patch", None, None),
            P("patch", None, None),
            P("patch", None),
            P("patch", None, None, None),
            P("patch", None, None),
            P("patch", None, None),
        ),
        out_specs=(P("patch", "rhs", None), P("patch", "rhs", None)),
        check_vma=False,
    )
```

```python
import jax
import jax.numpy as jnp
from jax import lax
from jax.experimental import pallas as pl
from jax.experimental.pallas import tpu as pltpu
from jax.sharding import PartitionSpec as P


HIGH = lax.Precision.HIGH
F32 = jnp.float32
BF16 = jnp.bfloat16
MIB = 1024 * 1024

K = 16
W = 384
E = 64
NB = 4
FL = 4
PD = 8
ROWS = PD * K

SMEM = pl.BlockSpec(memory_space=pltpu.SMEM)
VMEM = pl.BlockSpec(memory_space=pltpu.VMEM)
HBM = pl.BlockSpec(memory_space=pltpu.HBM)


def shape(*dims, dtype=F32):
    return jax.ShapeDtypeStruct(dims, dtype)


def nn(left, right):
    return jnp.dot(left, right, precision=HIGH, preferred_element_type=F32)


def exact(left, right):
    return jnp.dot(left, right, precision=lax.Precision.HIGHEST, preferred_element_type=F32)


def nt(left, right):
    return lax.dot_general(
        left, right, (((1,), (1,)), ((), ())), precision=HIGH, preferred_element_type=F32
    )


def iotas(rows, cols):
    return (
        lax.broadcasted_iota(jnp.int32, (rows, cols), 0),
        lax.broadcasted_iota(jnp.int32, (rows, cols), 1),
    )


def inverse(matrix):
    row, lane = iotas(K, 2 * K)
    eye = jnp.where(lane == row + K, 1.0, 0.0).astype(F32)
    work = jnp.concatenate([matrix, eye[:, K:]], axis=1)
    for i in range(0, K, 2):
        left = jnp.broadcast_to(work[:, i : i + 1], (K, 2 * K))
        right = jnp.broadcast_to(work[:, i + 1 : i + 2], (K, 2 * K))
        a, c = left[i : i + 1], left[i + 1 : i + 2]
        b, d = right[i : i + 1], right[i + 1 : i + 2]
        upper, lower = work[i : i + 1], work[i + 1 : i + 2]
        scale = 1.0 / (a * d - b * c)
        upper, lower = (d * upper - b * lower) * scale, (a * lower - c * upper) * scale
        rest = work - left * upper - right * lower
        work = jnp.where(row == i, upper, jnp.where(row == i + 1, lower, rest))
    return work[:, K:]


def small(left, right):
    terms = [left[:, k : k + 1] * right[k : k + 1, :] for k in range(K)]
    while len(terms) > 1:
        terms = [a + b for a, b in zip(terms[::2], terms[1::2])]
    return terms[0]


def tiled(matrix):
    wide = jnp.concatenate([matrix, jnp.zeros((K, ROWS - K), F32)], axis=1)
    for step in (K, 2 * K, 4 * K):
        wide = wide + pltpu.roll(wide, step, 1)
    return wide


def block_diagonal(matrix):
    wide = jnp.concatenate([tiled(matrix)] * PD, axis=0)
    row, lane = iotas(ROWS, ROWS)
    return jnp.where(row // K == lane // K, wide, 0.0)


def side_by_side(field):
    return jnp.concatenate([field[p * K : (p + 1) * K] for p in range(PD)], axis=1)


def fetch(near_ref, blocks_ref, sems):
    def start(p, carry):
        pltpu.make_async_copy(near_ref.at[p], blocks_ref.at[p], sems.at[p]).start()
        return carry

    lax.fori_loop(0, PD, start, 0)


def fetched(near_ref, blocks_ref, sems):
    def wait(p, carry):
        pltpu.make_async_copy(near_ref.at[p], blocks_ref.at[p], sems.at[p]).wait()
        return carry

    lax.fori_loop(0, PD, wait, 0)


def near_product(ids_ref, blocks_ref, rounded_ref):
    total = None
    for p in range(PD):
        fields = jnp.concatenate([rounded_ref[ids_ref[p, j]] for j in range(NB)], axis=1)
        pieces = [fields]
        if p:
            pieces.insert(0, jnp.zeros((p * K, NB * W), BF16))
        if p + 1 < PD:
            pieces.append(jnp.zeros(((PD - 1 - p) * K, NB * W), BF16))
        fields = jnp.concatenate(pieces, axis=0)
        blocks = jnp.concatenate([blocks_ref[p, j] for j in range(NB)], axis=1)
        part = lax.dot_general(
            blocks, fields, (((1,), (1,)), ((), ())), preferred_element_type=F32
        )
        total = part if total is None else total + part
    return total


def shifted(local_exp, shift_ref):
    return nt(local_exp, shift_ref[...].reshape(PD * E, E))


def far_product(patch_exp, down_ref):
    row, lane = iotas(ROWS, PD * E)
    wide = jnp.concatenate([patch_exp] * PD, axis=0)
    wide = jnp.where(row // K == lane // E, wide, 0.0)
    return nn(wide, down_ref[...].reshape(PD * E, W))


def expansion(chosen, table_ref):
    total = None
    for j in range(FL):
        moment = chosen[j]
        if moment.shape[0] < K:
            moment = jnp.concatenate([moment[:, :E], moment[:, E:]], axis=0)
        part = nt(moment[:, :E], table_ref[j])
        total = part if total is None else total + part
    return total


def summed(parts):
    while len(parts) > 1:
        parts = [a + b for a, b in zip(parts[::2], parts[1::2])]
    return parts[0]


def maps_kernel(up_ref, shift_ref, pick_ref, out_ref, pick_out):
    pick_out[...] = pick_ref[...]
    for p in range(PD):
        out_ref[:, p * W : (p + 1) * W] = nn(shift_ref[p], up_ref[p])


def moment_kernel(field_ref, up_ref, out_ref):
    moment = nt(side_by_side(field_ref[...].reshape(ROWS, W)), up_ref[...])
    message = jnp.concatenate([moment[: K // 2], moment[K // 2 :]], axis=1)
    for i in range(out_ref.shape[0]):
        out_ref[i] = message


def near_kernel(
    ids_ref, partner_ref, own_ref, beyond_ref, near_ref, out_ref, blocks_ref, rounded_ref, ids_smem, sems
):
    ids = pltpu.make_async_copy(ids_ref, ids_smem, sems.at[PD])
    ids.start()
    fetch(near_ref, blocks_ref, sems)
    for i, ref in enumerate((partner_ref, own_ref, beyond_ref)):
        rounded_ref[i * PD : (i + 1) * PD] = ref[...].astype(BF16)
    ids.wait()
    fetched(near_ref, blocks_ref, sems)
    out_ref[...] = near_product(ids_smem, blocks_ref, rounded_ref).T


def image_kernel(
    pick_ref, gathered_ref, near_ref, field_ref, up_ref, table_ref, shift_ref, down_ref,
    image_out, local_out, out_ref,
):
    count = gathered_ref.shape[0]
    chosen = [
        summed([gathered_ref[c] * pick_ref[j * count + c : j * count + c + 1] for c in range(count)])
        for j in range(FL)
    ]
    local_exp = expansion(chosen, table_ref)
    local_out[...] = jnp.concatenate([local_exp, jnp.zeros((K, E), F32)], axis=1)
    image = near_ref[...] + far_product(shifted(local_exp, shift_ref), down_ref)
    image_out[...] = image.reshape(PD, K, W)
    image = side_by_side(image)
    moment = nt(image, up_ref[...])
    both = jnp.concatenate([side_by_side(field_ref[...].reshape(ROWS, W)), image], axis=0)
    grams = nt(both, both)
    message = jnp.concatenate(
        [moment, grams[K:, :], grams[:K, :]], axis=1
    )
    for i in range(out_ref.shape[0]):
        out_ref[i] = message


def total_of(gathered_ref):
    return summed([gathered_ref[i] for i in range(gathered_ref.shape[0])])


def direction_kernel(
    ids_ref, far_ref, gathered_ref, total_ref, f_partner, f_own, f_beyond, q_partner, q_own, q_beyond,
    local_ref, table_ref, shift_ref, down_ref, near_ref,
    out_ref, direction_out, image_out, alpha_out,
    blocks_ref, rounded_ref, ids_smem, far_smem, sems,
):
    ids = pltpu.make_async_copy(ids_ref, ids_smem, sems.at[PD])
    far_ids = pltpu.make_async_copy(far_ref, far_smem, sems.at[PD + 1])
    ids.start()
    far_ids.start()
    fetch(near_ref, blocks_ref, sems)
    total = total_ref[...]
    qr = total[:, E : E + K]
    qq = total[:, E + K : E + 2 * K]
    rr = total[:, E + 2 * K : E + 3 * K]
    rq = total[:, E + 3 * K :]
    curve_inv = inverse(0.5 * (qr + rq))
    rr_inv = inverse(rr)
    alpha = small(curve_inv, rr)
    alpha_t = small(rr, curve_inv)
    following = (
        rr - small(rq, alpha) - small(alpha_t, qr) + small(alpha_t, small(qq, alpha))
    )
    row, lane = iotas(K, K)
    lift_t = small(following, rr_inv) + jnp.where(row == lane, 1.0, 0.0)
    alpha_out[...] = jnp.concatenate([alpha_t, jnp.zeros((K, ROWS - K), F32)], axis=1)
    far_ids.wait()
    image_exp = expansion([gathered_ref[far_smem[0, j]] for j in range(FL)], table_ref)
    local_exp = small(lift_t, local_ref[:, :E]) - small(alpha_t, image_exp)
    far = far_product(shifted(local_exp, shift_ref), down_ref)

    coeffs = block_diagonal(-alpha_t)
    both = jnp.concatenate([block_diagonal(lift_t), coeffs], axis=1)
    for i, (f, q) in enumerate(((f_partner, q_partner), (f_own, q_own), (f_beyond, q_beyond))):
        pair = jnp.concatenate(
            [f[...].reshape(ROWS, W), q[...].reshape(ROWS, W)], axis=0
        )
        mixed = exact(both, pair)
        if i == 1:
            direction = mixed
            residual = f_own[...].reshape(ROWS, W) + exact(coeffs, q_own[...].reshape(ROWS, W))
        rounded_ref[i * PD : (i + 1) * PD] = mixed.astype(BF16).reshape(PD, K, W)
    direction_out[...] = direction
    ids.wait()
    fetched(near_ref, blocks_ref, sems)
    image = near_product(ids_smem, blocks_ref, rounded_ref)
    image = image.T + far
    image_out[...] = image
    residual = side_by_side(residual)
    grams = nt(
        jnp.concatenate([side_by_side(image), residual], axis=0),
        jnp.concatenate([side_by_side(direction), residual], axis=0),
    )
    message = jnp.concatenate([grams[:K, :K], grams[K:, K:]], axis=1)
    message = jnp.concatenate(
        [message[: K // 2], message[K // 2 :], jnp.zeros((K // 2, ROWS - 4 * K), F32)], axis=1
    )
    for i in range(out_ref.shape[0]):
        out_ref[i] = message


def own_coeffs(pick, coeffs_t):
    row, lane = iotas(K, ROWS)
    return jnp.where(row // 2 == lane // K, tiled(small(pick, coeffs_t)), 0.0)


def last_step_kernel(
    pick_ref, gathered_ref, alpha_ref, field_ref, image0_ref, direction_ref, image_ref,
    x_out, r_out,
):
    pick = pick_ref[...]
    field = field_ref[...].reshape(ROWS, W)
    row, lane = iotas(K, ROWS)
    mine = jnp.where(row // 2 == lane // K, tiled(pick), 0.0)
    coeffs0 = own_coeffs(pick, alpha_ref[:, :K])
    x = exact(coeffs0, field)
    r = exact(mine, field) - exact(coeffs0, image0_ref[...].reshape(ROWS, W))
    total = total_of(gathered_ref)
    total = jnp.concatenate([total[:, : 2 * K], total[:, 2 * K : 4 * K]], axis=0)
    qd = total[:, :K]
    alpha_t = small(total[:, K : 2 * K], inverse(0.5 * (qd + qd.T)))
    coeffs = own_coeffs(pick, alpha_t)
    x = x + nn(coeffs, direction_ref[...])
    r = r - nn(coeffs, image_ref[...])
    for p in range(PD):
        x_out[p] = x[2 * p : 2 * p + 2]
        r_out[p] = r[2 * p : 2 * p + 2]


def call(kernel, in_specs, out_shape, scratch=(), limit=24, cost=1):
    many = isinstance(out_shape, (tuple, list))
    return pl.pallas_call(
        kernel,
        in_specs=in_specs,
        out_specs=tuple(VMEM for _ in out_shape) if many else VMEM,
        out_shape=out_shape,
        scratch_shapes=scratch,
        compiler_params=pltpu.CompilerParams(vmem_limit_bytes=limit * MIB),
        cost_estimate=pl.CostEstimate(flops=cost * 1_000_000, bytes_accessed=1_000_000, transcendentals=0),
    )


NEAR_SCRATCH = (
    pltpu.VMEM((PD, NB, W, W), BF16),
    pltpu.VMEM((3 * PD, K, W), BF16),
    pltpu.SMEM((PD, NB), jnp.int32),
)


def swap(array, axis):
    return lax.all_to_all(array, axis, 0, 0, tiled=True)


def halo(block, axis):
    count = lax.axis_size(axis)
    partner = lax.ppermute(block, axis, [(i, i ^ 1) for i in range(count)])
    beyond = lax.ppermute(
        block, axis, [(i, (i + (1 if i % 2 else -1)) % count) for i in range(count)]
    )
    return partner, beyond


def on_device(
    rhs_vectors,
    near_blocks,
    neighbours,
    up_maps,
    shift_up,
    far_lists,
    translations,
    shift_down,
    down_maps,
):
    count = lax.axis_size("patch")
    depth = lax.axis_size("rhs")
    place = lax.axis_index("rhs").astype(jnp.int32)
    cell = lax.axis_index("patch")
    owner = neighbours // PD
    slot = jnp.where(owner == cell, 1, jnp.where(owner == cell ^ 1, 0, 2))
    ids = (slot * PD + neighbours % PD).astype(jnp.int32)

    message = jnp.broadcast_to(rhs_vectors[None], (depth, *rhs_vectors.shape))
    parts = swap(message, "rhs")
    field = parts.transpose(1, 2, 0, 3).reshape(PD, K, W)

    row, lane = jnp.arange(K)[:, None], jnp.arange(K)[None, :]
    pick_column = (lane == (row % 2) * PD + place).astype(F32)
    pick_cell = (far_lists[0][:, None] == jnp.arange(count)[None, :]).astype(F32)
    pick_cell = jnp.broadcast_to(pick_cell.reshape(FL * count, 1), (FL * count, 2 * E))

    up, pick_column = call(maps_kernel, [VMEM] * 3, (shape(E, PD * W), shape(K, K)))(
        up_maps, shift_up, pick_column
    )
    table = translations[0]
    down = down_maps.transpose(0, 2, 1)

    f_partner, f_beyond = halo(field, "patch")
    message = call(moment_kernel, [VMEM] * 2, shape(count, K // 2, ROWS))(field, up)
    gathered = swap(message, "patch")
    near = call(
        near_kernel,
        [VMEM] * 4 + [HBM],
        shape(ROWS, W),
        (*NEAR_SCRATCH, pltpu.SemaphoreType.DMA((PD + 1,))),
        limit=48,
    )(
        ids, f_partner, field, f_beyond, near_blocks
    )
    image, local_exp, message = call(
        image_kernel,
        [VMEM] * 8,
        (shape(PD, K, W), shape(K, 2 * E), shape(count, K, ROWS)),
    )(pick_cell, gathered, near, field, up, table, shift_down, down)

    q_partner, q_beyond = halo(image, "patch")
    gathered = swap(message, "patch")
    total = gathered.sum(axis=0)
    message, direction, image1, alpha = call(
        direction_kernel,
        [VMEM] * 14 + [HBM],
        (shape(count, K // 2, ROWS), shape(ROWS, W), shape(ROWS, W), shape(K, ROWS)),
        (*NEAR_SCRATCH, pltpu.SMEM((1, FL), jnp.int32), pltpu.SemaphoreType.DMA((PD + 2,))),
        limit=48,
    )(
        ids, far_lists, gathered, total, f_partner, field, f_beyond, q_partner, image, q_beyond,
        local_exp, table, shift_down, down, near_blocks,
    )

    gathered = swap(message, "patch")
    return call(last_step_kernel, [VMEM] * 7, (shape(PD, 2, W),) * 2)(
        pick_column, gathered, alpha, field, image, direction, image1
    )


def solution(mesh):
    return jax.shard_map(
        on_device,
        mesh=mesh,
        in_specs=(
            P("patch", "rhs", None),
            P("patch", None, None, None),
            P("patch", None),
            P("patch", None, None),
            P("patch", None, None),
            P("patch", None),
            P("patch", None, None, None),
            P("patch", None, None),
            P("patch", None, None),
        ),
        out_specs=(P("patch", "rhs", None), P("patch", "rhs", None)),
        check_vma=False,
    )
```
